32 devices in a mesh: far: 4 (over z), near: 8 (over y, x, core).
Axes of the slice: x: 2, y: 2, z: 4, core: 2. Of those that a mesh axis runs over, the one named last changes fastest.
Arguments:
- state_real: float32 [4, 8, 2, 128, 128], P('far', 'near'), may hold values from -5 to 5
- state_imag: float32 [4, 8, 2, 128, 128], P('far', 'near'), may hold values from -5 to 5
- gate_real: float32 [2, 4, 3, 128, 128], replicated, may hold values from -0.375 to 0.375
- gate_imag: float32 [2, 4, 3, 128, 128], replicated, may hold values from -0.375 to 0.375
Outputs:
- final_real: float32 [4, 8, 2, 128, 128], P('far', 'near')
- final_imag: float32 [4, 8, 2, 128, 128], P('far', 'near')
The draws below stay inside these ranges and needn't reach their ends.
All inputs are finite; a program needn't handle non-finite values.
Results may differ from the reference program's by a relative error of at most 0.000071.
Values sent between devices are 32-bit elements; how exact they have to be, the bound alone decides.
A program may use at most 64 MiB of HBM per device.

```python
import jax
import jax.numpy as jnp
from jax import lax

GATE = 128
HIGH = 2
ROUNDS = 2
SECTIONS = 4
DEPTH = 3
N_FAR = 4
N_NEAR = 8


def shard_levels(key, shape, cuts, low, high):
    level = 1.0
    for axis_at, parts in cuts:
        heights = jax.random.uniform(jax.random.fold_in(jax.random.fold_in(key, 6), axis_at), (parts,), jnp.float32, low / len(cuts), high / len(cuts))
        level = level * jnp.repeat(jnp.exp(heights), shape[axis_at] // parts).reshape((-1,) + (1,) * (len(shape) - 1 - axis_at))
    return level


def noise(rng, dims, spread, most, cuts=(), kind=jnp.bfloat16):
    array = spread * jax.random.normal(rng, dims, jnp.float32)
    if cuts:
        array = array * shard_levels(rng, dims, cuts, -0.22, 0.18)
    return jnp.clip(array, -most, most).astype(kind)


def setup_inputs(seed: int = 0) -> dict:
    arg_keys = jax.random.split(jax.random.key(seed), 5)
    return {
        "state_real": noise(arg_keys[0], (N_FAR, N_NEAR, HIGH, GATE, GATE), 0.7, 5.0, ((0, 4), (1, 8)), jnp.float32),
        "state_imag": noise(arg_keys[1], (N_FAR, N_NEAR, HIGH, GATE, GATE), 0.7, 5.0, ((0, 4), (1, 8)), jnp.float32),
        "gate_real": noise(arg_keys[2], (ROUNDS, SECTIONS, DEPTH, GATE, GATE), (2 * GATE) ** -0.5, 0.375, (), jnp.float32),
        "gate_imag": noise(arg_keys[3], (ROUNDS, SECTIONS, DEPTH, GATE, GATE), (2 * GATE) ** -0.5, 0.375, (), jnp.float32),
    }


def gate_low(x, g):
    return jnp.einsum('...l,jl->...j', x, g, precision=lax.Precision.HIGHEST, preferred_element_type=jnp.float32)


def gate_mid(x, g):
    return jnp.einsum('...ml,jm->...jl', x, g, precision=lax.Precision.HIGHEST, preferred_element_type=jnp.float32)


def gate_top(x, g):
    high, width, lows = x.shape[-3], x.shape[-2], x.shape[-1]
    upper = g.shape[0] // high
    lead = x.shape[:-3]
    viewed = x.reshape(lead + (high, upper, width // upper, lows))
    matrix = g.reshape((g.shape[0], high, upper))
    out = jnp.einsum('...hkrl,jhk->...jrl', viewed, matrix, precision=lax.Precision.HIGHEST, preferred_element_type=jnp.float32)
    return out.reshape(lead + (high, width, lows))


def complex_gate(form, real, imag, greal, gimag):
    new_real = form(real, greal) - form(imag, gimag)
    new_imag = form(imag, greal) + form(real, gimag)
    return new_real, new_imag


def swap_far(x):
    nfar, nnear, high, width, lows = x.shape
    y = x.reshape((nfar, nnear, nfar, high * width // nfar, lows))
    return jnp.swapaxes(y, 0, 2).reshape(x.shape)


def swap_mid(x):
    nfar, nnear, high, width, lows = x.shape
    y = x.reshape((nfar, nnear, high, nnear, width // nnear, lows))
    return jnp.swapaxes(y, 1, 3).reshape(x.shape)


def swap_low(x):
    nfar, nnear, high, width, lows = x.shape
    y = x.reshape((nfar, nnear, high, width, nnear, lows // nnear))
    return jnp.swapaxes(y, 1, 4).reshape(x.shape)


def swap_top(x):
    nfar, nnear, high, width, lows = x.shape
    y = x.reshape((nfar, nnear, nnear, high * width // nnear, lows))
    return jnp.swapaxes(y, 1, 2).reshape(x.shape)


def reference(state_real, state_imag, gate_real, gate_imag):
    real, imag = state_real, state_imag
    swaps = (swap_far, swap_mid, swap_low, swap_top)
    forms = (gate_low, gate_mid, gate_top)
    for rnd in range(ROUNDS):
        for section in range(4):
            real = swaps[section](real)
            imag = swaps[section](imag)
            for which in range(3):
                real, imag = complex_gate(forms[which], real, imag, gate_real[rnd, section, which], gate_imag[rnd, section, which])
    return real, imag
```

```python
import functools

import jax
import jax.numpy as jnp
from jax import lax
from jax.experimental import pallas as pl
from jax.experimental.pallas import tpu as pltpu
from jax.sharding import PartitionSpec as P


def gate_low(x, g):
    return jnp.einsum(
        "...l,jl->...j", x, g, precision=lax.Precision.HIGHEST, preferred_element_type=jnp.float32
    )


def gate_mid(x, g):
    return jnp.einsum(
        "...ml,jm->...jl", x, g, precision=lax.Precision.HIGHEST, preferred_element_type=jnp.float32
    )


def gate_top(x, g):
    high, width, lows = (x.shape[-3], x.shape[-2], x.shape[-1])
    upper = g.shape[0] // high
    lead = x.shape[:-3]
    viewed = x.reshape(lead + (high, upper, width // upper, lows))
    matrix = g.reshape((g.shape[0], high, upper))
    out = jnp.einsum(
        "...hkrl,jhk->...jrl",
        viewed,
        matrix,
        precision=lax.Precision.HIGHEST,
        preferred_element_type=jnp.float32,
    )
    return out.reshape(lead + (high, width, lows))


def complex_gate(form, real, imag, greal, gimag):
    new_real = form(real, greal) - form(imag, gimag)
    new_imag = form(imag, greal) + form(real, gimag)
    return (new_real, new_imag)


def merged_rows(x):
    return x.reshape((1, 1, x.shape[2] * x.shape[3], x.shape[4]))


def on_device(state_real, state_imag, gate_real, gate_imag):
    real, imag = (state_real, state_imag)
    forms = (gate_low, gate_mid, gate_top)
    shape = state_real.shape
    for rnd in range(gate_real.shape[0]):
        for section in range(4):
            if section == 2:
                order = [1, 0, 2]
            else:
                order = [0, 1, 2]
            early = []
            later = order[len(early) :]
            pair = (real, imag)
            if section == 0:
                moved = (
                    lax.all_to_all(
                        merged_rows(pair[0]), "far", split_axis=2, concat_axis=2, tiled=True
                    ),
                    lax.all_to_all(
                        merged_rows(pair[1]), "far", split_axis=2, concat_axis=2, tiled=True
                    ),
                )
                pair = (moved[0].reshape(shape), moved[1].reshape(shape))
            elif section == 1:
                pair = (
                    lax.all_to_all(pair[0], "near", split_axis=3, concat_axis=3, tiled=True),
                    lax.all_to_all(pair[1], "near", split_axis=3, concat_axis=3, tiled=True),
                )
            elif section == 2:
                pair = (
                    lax.all_to_all(pair[0], "near", split_axis=4, concat_axis=4, tiled=True),
                    lax.all_to_all(pair[1], "near", split_axis=4, concat_axis=4, tiled=True),
                )
            else:
                moved = (
                    lax.all_to_all(
                        merged_rows(pair[0]), "near", split_axis=2, concat_axis=2, tiled=True
                    ),
                    lax.all_to_all(
                        merged_rows(pair[1]), "near", split_axis=2, concat_axis=2, tiled=True
                    ),
                )
                pair = (moved[0].reshape(shape), moved[1].reshape(shape))
            for which in later:
                pair = complex_gate(
                    forms[which],
                    pair[0],
                    pair[1],
                    gate_real[rnd, section, which],
                    gate_imag[rnd, section, which],
                )
            real, imag = pair
    return (real, imag)


def parts(x):
    first = x.astype(jnp.bfloat16)
    return first, (x - first.astype(jnp.float32)).astype(jnp.bfloat16)


def dot(a, b, dims=((1,), (0,))):
    def product(x, y):
        return lax.dot_general(x, y, (dims, ((), ())), preferred_element_type=jnp.float32)

    return product(a[0], b[0]) + (product(a[0], b[1]) + product(a[1], b[0]))


def product(a, b):
    n = a[0].shape[0]
    w = b[0].shape[1]
    out = dot(parts(jnp.concatenate(a, axis=0)), parts(jnp.concatenate(b, axis=1)))
    return out[:n, :w] - out[n:, w:], out[n:, :w] + out[:n, w:]


def trade(x, row, lane, count):
    rows, lanes = x.shape
    at = lax.broadcasted_iota(jnp.int32, (row, lanes), 1)
    for _ in range(count):
        low = lax.rem(lax.div(at, lane), 2) == 0
        pieces = []
        for start in range(0, rows, 2 * row):
            a, b = x[start : start + row], x[start + row : start + 2 * row]
            pieces.append(jnp.where(low, a, pltpu.roll(b, lane, 1)))
            pieces.append(jnp.where(low, pltpu.roll(a, lanes - lane, 1), b))
        x = jnp.concatenate(pieces, axis=0)
        row, lane, at = row // 2, lane // 2, at[: row // 2]
    return x


def kernel(sizes, sr_hbm, si_hbm, gr_hbm, gi_hbm, or_ref, oi_ref, *scratch):
    nfar, nnear, high, order, lows = sizes
    (
        st_ref, gr_ref, gi_ref, kf_ref, km_ref, w_ref,
        send0, send1, send2, send3, recv0, recv1, recv2, recv3,
        send_sem, recv_sem, load_sem,
    ) = scratch
    sends, recvs = (send0, send1, send2, send3), (recv0, recv1, recv2, recv3)
    far, near = lax.axis_index("far"), lax.axis_index("near")
    upper = order // high
    rest = order // upper
    rows = high * order
    chunks = 2
    fine = lows // chunks // nnear
    half = lows // chunks

    barrier = pltpu.get_barrier_semaphore()
    for k in range(1, nfar):
        pl.semaphore_signal(
            barrier, inc=1, device_id=(lax.rem(far + k, nfar), near), device_id_type=pl.DeviceIdType.MESH
        )
    for k in range(1, nnear):
        pl.semaphore_signal(
            barrier, inc=1, device_id=(far, lax.rem(near + k, nnear)), device_id_type=pl.DeviceIdType.MESH
        )
    first = [
        pltpu.make_async_copy(gr_hbm.at[0, pl.ds(0, 2), 0], gr_ref.at[0, pl.ds(0, 2), 0], load_sem.at[0]),
        pltpu.make_async_copy(gi_hbm.at[0, pl.ds(0, 2), 0], gi_ref.at[0, pl.ds(0, 2), 0], load_sem.at[1]),
        pltpu.make_async_copy(sr_hbm, st_ref.at[0], load_sem.at[2]),
        pltpu.make_async_copy(si_hbm, st_ref.at[1], load_sem.at[3]),
    ]
    others = []
    at = 4
    for rnd in range(2):
        for hbm, ref in ((gr_hbm, gr_ref), (gi_hbm, gi_ref)):
            pieces = [(pl.ds(0, 4), pl.ds(1, 2))]
            pieces += [(pl.ds(2, 2), pl.ds(0, 1))] if rnd == 0 else [(pl.ds(0, 4), pl.ds(0, 1))]
            for s, g in pieces:
                others.append(pltpu.make_async_copy(hbm.at[rnd, s, g], ref.at[rnd, s, g], load_sem.at[at]))
                at += 1
    for load in first + others:
        load.start()

    pending = []

    def launch(stage, c):
        n, me = (nfar, far) if stage % 2 == 0 else (nnear, near)
        source, target = sends[stage].at[c], recvs[stage].at[c]
        for k in ([2, 3, 1] if n == 4 else [6, 7, 5, 2, 3, 4, 1] if n == 8 else range(1, n)):
            to = lax.rem(me + k, n)
            copy = pltpu.make_async_remote_copy(
                src_ref=source.at[to],
                dst_ref=target.at[me],
                send_sem=send_sem.at[stage, c, k],
                recv_sem=recv_sem.at[stage, c, k],
                device_id=(to, near) if stage % 2 == 0 else (far, to),
                device_id_type=pl.DeviceIdType.MESH,
            )
            copy.start()
            pending.append(copy)
        target[me] = source[me]

    def arrive(stage, c):
        n, me = (nfar, far) if stage % 2 == 0 else (nnear, near)
        target = recvs[stage].at[c]
        for k in range(1, n):
            origin = lax.rem(me + n - k, n)
            pltpu.make_async_remote_copy(
                src_ref=target.at[origin],
                dst_ref=target.at[origin],
                send_sem=send_sem.at[stage, c, k],
                recv_sem=recv_sem.at[stage, c, k],
                device_id=(origin, near) if stage % 2 == 0 else (far, origin),
                device_id_type=pl.DeviceIdType.MESH,
            ).wait_recv()

    def gate(s, which):
        return gr_ref[s // 4, s % 4, which], gi_ref[s // 4, s % 4, which]

    def finer(x):
        return jnp.concatenate(
            [
                x[(b * chunks + c) * fine : (b * chunks + c + 1) * fine]
                for c in range(chunks)
                for b in range(nnear)
            ],
            axis=0,
        )

    def split_rows(re, im):
        re, im = finer(re), finer(im)
        left, right = [], []
        for c in range(chunks):
            piece = slice(c * half, (c + 1) * half)
            left += [re[piece], im[piece]]
            right += [-im[piece], re[piece]]
        return jnp.concatenate([jnp.concatenate(left, axis=0), jnp.concatenate(right, axis=0)], axis=1)

    def chunked_columns(x):
        return jnp.concatenate([finer(x[:lows])[:half], finer(x[lows:])[:half],
                                finer(x[:lows])[half:], finer(x[lows:])[half:]], axis=0)

    def put_low(at, re, im, finely):
        if finely:
            wide = split_rows(re, im)
        else:
            wide = jnp.concatenate(
                [jnp.concatenate([re, im], axis=0), jnp.concatenate([-im, re], axis=0)], axis=1
            )
        w_ref[at, 0], w_ref[at, 1] = parts(chunked_columns(wide.T))

    def tops_after_mids(s):
        tr, ti = gate(s, 2)
        left = parts(
            jnp.concatenate(
                [jnp.concatenate([tr, -ti], axis=1), jnp.concatenate([ti, tr], axis=1)], axis=0
            )
        )
        zero = jnp.zeros((upper, order), jnp.float32)
        for t in range(rest):
            blocks = []
            for ref in (gr_ref, gi_ref):
                mid = ref[s // 4, s % 4, 1, pl.ds(t, upper, stride=rest), :]
                for h in range(high):
                    blocks.append(jnp.concatenate([mid if g == h else zero for g in range(high)], axis=1))
            out = dot(left, parts(jnp.concatenate(blocks, axis=0)))
            for c in range(2):
                for h in range(high):
                    for g in range(high):
                        kf_ref[c, g, h, pl.ds(t, upper, stride=rest), :] = out[
                            c * order + h * upper : c * order + (h + 1) * upper, g * order : (g + 1) * order
                        ]
        return tuple(
            jnp.concatenate([kf_ref[c, g].reshape(rows, order) for g in range(high)], axis=1) for c in range(2)
        )

    def put_high(at, pair):
        km_ref[at, 0], km_ref[at, 1] = parts(jnp.concatenate(pair, axis=0))

    def high_of(at):
        return km_ref[at, 0], km_ref[at, 1]

    lane = lax.broadcasted_iota(jnp.int32, (rows, lows), 1)
    sign = jnp.where(lane < half, -1.0, 1.0)

    def apply(at, x):
        out = dot(high_of(at), parts(x))
        return out[:rows] + sign * pltpu.roll(out[rows:], half, 1)

    first[0].wait()
    first[1].wait()
    l1, l0 = gate(1, 0), gate(0, 0)
    low = parts(split_rows(*product(l1, l0)))
    first[2].wait()
    first[3].wait()
    state = jnp.concatenate([st_ref[0], st_ref[1]], axis=1)
    state = dot(parts(state), low, ((1,), (1,)))
    for c in range(chunks):
        sends[0][c] = state[:, c * lows : (c + 1) * lows].reshape(nfar, rows // nfar, lows)
    pl.semaphore_wait(barrier, nfar - 1 + nnear - 1)
    for c in range(chunks):
        launch(0, c)

    for load in others:
        load.wait()
    put_high(0, tops_after_mids(0))
    put_high(1, tops_after_mids(2))
    k1 = tops_after_mids(1)
    out = dot(high_of(1), parts(jnp.concatenate(k1, axis=1)))
    put_high(1, (out[:rows, :rows] - out[rows:, rows:], out[rows:, :rows] + out[:rows, rows:]))
    put_high(2, tops_after_mids(3))

    count = order // nnear
    for c in range(chunks):
        arrive(0, c)
        x = apply(0, recvs[0][c].reshape(rows, lows))
        for b in range(nnear):
            for h in range(high):
                sends[1][c, b, h] = x[h * order + b * count : h * order + (b + 1) * count]
        launch(1, c)
        if c == 0:
            put_high(3, tops_after_mids(4))

    for c in range(chunks):
        arrive(1, c)
        x = jnp.concatenate([recvs[1][c, :, h].reshape(order, lows) for h in range(high)], axis=0)
        x = trade(apply(1, x), rows // 2, half // 2, 3)
        sends[2][c] = apply(2, x).reshape(nfar, rows // nfar, lows)
        launch(2, c)

    put_high(4, tops_after_mids(6))
    k5 = tops_after_mids(5)
    out = dot(high_of(4), parts(jnp.concatenate(k5, axis=1)))
    put_high(4, (out[:rows, :rows] - out[rows:, rows:], out[rows:, :rows] + out[:rows, rows:]))
    put_low(0, *product(gate(5, 0), product(gate(4, 0), product(gate(3, 0), gate(2, 0)))), True)

    for c in range(chunks):
        arrive(2, c)
        x = apply(3, recvs[2][c].reshape(rows, lows))
        x = trade(x, rows // 4, half // 2, 3)
        sends[3][c] = apply(4, x).reshape(nnear, rows // nnear, lows)
        launch(3, c)

    put_high(5, tops_after_mids(7))
    put_low(1, *product(gate(7, 0), gate(6, 0)), False)

    begun = []
    for c in range(chunks):
        arrive(3, c)
        x = trade(recvs[3][c].reshape(rows, lows), rows // 2, half // 2, 3)
        piece = slice(c * lows, (c + 1) * lows)
        begun.append(dot(parts(x), (w_ref[0, 0, piece], w_ref[0, 1, piece])))
    x = begun[0] + begun[1]
    x = jnp.concatenate([trade(x[:, c * lows : (c + 1) * lows], rows // 2, half // 2, 3) for c in range(chunks)], axis=1)
    x = dot(parts(x), (w_ref[1, 0], w_ref[1, 1]))
    out = dot(high_of(5), parts(x))
    or_ref[...] = out[:rows, :lows] - out[rows:, lows:]
    oi_ref[...] = out[rows:, :lows] + out[:rows, lows:]
    for copy in pending:
        copy.wait_send()


def one_kernel(nfar, nnear, state_real, state_imag, gate_real, gate_imag):
    shape = state_real.shape
    high, order, lows = shape[2:]
    rows = high * order
    blocks = (
        (2, nfar, rows // nfar, lows),
        (2, nnear, high, order // nnear, lows),
        (2, nfar, rows // nfar, lows),
        (2, nnear, rows // nnear, lows),
    )
    buffers = [pltpu.VMEM(block, jnp.float32) for block in blocks]
    vmem = pl.BlockSpec(memory_space=pltpu.VMEM)
    anywhere = pl.BlockSpec(memory_space=pl.ANY)
    result = pltpu.VMEM((rows, lows), jnp.float32)
    real, imag = pl.pallas_call(
        functools.partial(kernel, (nfar, nnear, high, order, lows)),
        out_shape=(result, result),
        in_specs=[anywhere] * 4,
        out_specs=(vmem, vmem),
        scratch_shapes=[
            pltpu.VMEM((2, rows, lows), jnp.float32),
            pltpu.VMEM(gate_real.shape, jnp.float32),
            pltpu.VMEM(gate_imag.shape, jnp.float32),
            pltpu.VMEM((2, high, high, order, order), jnp.float32),
            pltpu.VMEM((6, 2, 2 * rows, rows), jnp.bfloat16),
            pltpu.VMEM((2, 2, 2 * lows, 2 * lows), jnp.bfloat16),
        ]
        + buffers
        + buffers
        + [
            pltpu.SemaphoreType.DMA((4, 2, max(nfar, nnear))),
            pltpu.SemaphoreType.DMA((4, 2, max(nfar, nnear))),
            pltpu.SemaphoreType.DMA((12,)),
        ],
        compiler_params=pltpu.CompilerParams(collective_id=0, has_side_effects=True),
    )(
        state_real.reshape(rows, lows),
        state_imag.reshape(rows, lows),
        gate_real,
        gate_imag,
    )
    return real.reshape(shape), imag.reshape(shape)


def solution(mesh):
    nfar, nnear = mesh.shape["far"], mesh.shape["near"]

    def body(state_real, state_imag, gate_real, gate_imag):
        high, order, lows = state_real.shape[2:]
        fits = nfar == high * high and nnear == high * nfar and order == lows and gate_real.shape[0] == 2
        fits = fits and high == 2 and lows // nnear // 2 == 8
        if not fits:
            return on_device(state_real, state_imag, gate_real, gate_imag)
        return one_kernel(nfar, nnear, state_real, state_imag, gate_real, gate_imag)

    return jax.shard_map(
        body,
        mesh=mesh,
        in_specs=(P("far", "near", None, None, None), P("far", "near", None, None, None), P(), P()),
        out_specs=(P("far", "near", None, None, None), P("far", "near", None, None, None)),
        check_vma=False,
    )
```

```python
import functools

import jax
import jax.numpy as jnp
from jax import lax
from jax.experimental import pallas as pl
from jax.experimental.pallas import tpu as pltpu
from jax.sharding import PartitionSpec as P


def gate_low(x, g):
    return jnp.einsum(
        "...l,jl->...j", x, g, precision=lax.Precision.HIGHEST, preferred_element_type=jnp.float32
    )


def gate_mid(x, g):
    return jnp.einsum(
        "...ml,jm->...jl", x, g, precision=lax.Precision.HIGHEST, preferred_element_type=jnp.float32
    )


def gate_top(x, g):
    high, width, lows = (x.shape[-3], x.shape[-2], x.shape[-1])
    upper = g.shape[0] // high
    lead = x.shape[:-3]
    viewed = x.reshape(lead + (high, upper, width // upper, lows))
    matrix = g.reshape((g.shape[0], high, upper))
    out = jnp.einsum(
        "...hkrl,jhk->...jrl",
        viewed,
        matrix,
        precision=lax.Precision.HIGHEST,
        preferred_element_type=jnp.float32,
    )
    return out.reshape(lead + (high, width, lows))


def complex_gate(form, real, imag, greal, gimag):
    new_real = form(real, greal) - form(imag, gimag)
    new_imag = form(imag, greal) + form(real, gimag)
    return (new_real, new_imag)


def merged_rows(x):
    return x.reshape((1, 1, x.shape[2] * x.shape[3], x.shape[4]))


def on_device(state_real, state_imag, gate_real, gate_imag):
    real, imag = (state_real, state_imag)
    forms = (gate_low, gate_mid, gate_top)
    shape = state_real.shape
    for rnd in range(gate_real.shape[0]):
        for section in range(4):
            if section == 2:
                order = [1, 0, 2]
            else:
                order = [0, 1, 2]
            early = []
            later = order[len(early) :]
            pair = (real, imag)
            if section == 0:
                moved = (
                    lax.all_to_all(
                        merged_rows(pair[0]), "far", split_axis=2, concat_axis=2, tiled=True
                    ),
                    lax.all_to_all(
                        merged_rows(pair[1]), "far", split_axis=2, concat_axis=2, tiled=True
                    ),
                )
                pair = (moved[0].reshape(shape), moved[1].reshape(shape))
            elif section == 1:
                pair = (
                    lax.all_to_all(pair[0], "near", split_axis=3, concat_axis=3, tiled=True),
                    lax.all_to_all(pair[1], "near", split_axis=3, concat_axis=3, tiled=True),
                )
            elif section == 2:
                pair = (
                    lax.all_to_all(pair[0], "near", split_axis=4, concat_axis=4, tiled=True),
                    lax.all_to_all(pair[1], "near", split_axis=4, concat_axis=4, tiled=True),
                )
            else:
                moved = (
                    lax.all_to_all(
                        merged_rows(pair[0]), "near", split_axis=2, concat_axis=2, tiled=True
                    ),
                    lax.all_to_all(
                        merged_rows(pair[1]), "near", split_axis=2, concat_axis=2, tiled=True
                    ),
                )
                pair = (moved[0].reshape(shape), moved[1].reshape(shape))
            for which in later:
                pair = complex_gate(
                    forms[which],
                    pair[0],
                    pair[1],
                    gate_real[rnd, section, which],
                    gate_imag[rnd, section, which],
                )
            real, imag = pair
    return (real, imag)


def parts(x):
    first = x.astype(jnp.bfloat16)
    return first, (x - first.astype(jnp.float32)).astype(jnp.bfloat16)


def dot(a, b, dims=((1,), (0,))):
    def product(x, y):
        return lax.dot_general(x, y, (dims, ((), ())), preferred_element_type=jnp.float32)

    return product(a[0], b[0]) + (product(a[0], b[1]) + product(a[1], b[0]))


def product(a, b):
    n = a[0].shape[0]
    w = b[0].shape[1]
    out = dot(parts(jnp.concatenate(a, axis=0)), parts(jnp.concatenate(b, axis=1)))
    return out[:n, :w] - out[n:, w:], out[n:, :w] + out[:n, w:]


def trade(x, row, lane, count):
    rows, lanes = x.shape
    at = lax.broadcasted_iota(jnp.int32, (row, lanes), 1)
    for _ in range(count):
        low = lax.rem(lax.div(at, lane), 2) == 0
        pieces = []
        for start in range(0, rows, 2 * row):
            a, b = x[start : start + row], x[start + row : start + 2 * row]
            pieces.append(jnp.where(low, a, pltpu.roll(b, lane, 1)))
            pieces.append(jnp.where(low, pltpu.roll(a, lanes - lane, 1), b))
        x = jnp.concatenate(pieces, axis=0)
        row, lane, at = row // 2, lane // 2, at[: row // 2]
    return x


def kernel(sizes, sr_hbm, si_hbm, gr_hbm, gi_hbm, or_ref, oi_ref, *scratch):
    nfar, nnear, high, order, lows = sizes
    (
        st_ref, lr_ref, li_ref, gr_ref, gi_ref, kf_ref, km_ref, w_ref,
        send0, send1, send2, send3, recv0, recv1, recv2, recv3,
        send_sem, recv_sem, load_sem,
    ) = scratch
    sends, recvs = (send0, send1, send2, send3), (recv0, recv1, recv2, recv3)
    far, near = lax.axis_index("far"), lax.axis_index("near")
    upper = order // high
    rest = order // upper
    rows = high * order
    chunks = 2
    fine = lows // chunks // nnear
    half = lows // chunks

    barrier = pltpu.get_barrier_semaphore()
    for k in range(1, nfar):
        pl.semaphore_signal(
            barrier, inc=1, device_id=(lax.rem(far + k, nfar), near), device_id_type=pl.DeviceIdType.MESH
        )
    for k in range(1, nnear):
        pl.semaphore_signal(
            barrier, inc=1, device_id=(far, lax.rem(near + k, nnear)), device_id_type=pl.DeviceIdType.MESH
        )
    first = [
        pltpu.make_async_copy(gr_hbm.at[0, pl.ds(0, 2), 0], lr_ref, load_sem.at[0]),
        pltpu.make_async_copy(gi_hbm.at[0, pl.ds(0, 2), 0], li_ref, load_sem.at[1]),
        pltpu.make_async_copy(sr_hbm, st_ref.at[0], load_sem.at[2]),
        pltpu.make_async_copy(si_hbm, st_ref.at[1], load_sem.at[3]),
    ]
    others = [
        pltpu.make_async_copy(gr_hbm, gr_ref, load_sem.at[4]),
        pltpu.make_async_copy(gi_hbm, gi_ref, load_sem.at[5]),
    ]
    for load in first + others:
        load.start()

    def launch(stage, c):
        n, me = (nfar, far) if stage % 2 == 0 else (nnear, near)
        source, target = sends[stage].at[c], recvs[stage].at[c]
        for k in ([2, 3, 1] if n == 4 else [6, 7, 5, 2, 3, 4, 1] if n == 8 else range(1, n)):
            to = lax.rem(me + k, n)
            copy = pltpu.make_async_remote_copy(
                src_ref=source.at[to],
                dst_ref=target.at[me],
                send_sem=send_sem.at[stage],
                recv_sem=recv_sem.at[stage, c],
                device_id=(to, near) if stage % 2 == 0 else (far, to),
                device_id_type=pl.DeviceIdType.MESH,
            )
            copy.start()
        target[me] = source[me]

    def arrive(stage, c):
        n = nfar if stage % 2 == 0 else nnear
        landed = recvs[stage].at[c, pl.ds(0, n - 1)]
        pltpu.make_async_copy(landed, landed, recv_sem.at[stage, c]).wait()

    def gate(s, which):
        return gr_ref[s // 4, s % 4, which], gi_ref[s // 4, s % 4, which]

    def finer(x):
        return jnp.concatenate(
            [
                x[(b * chunks + c) * fine : (b * chunks + c + 1) * fine]
                for c in range(chunks)
                for b in range(nnear)
            ],
            axis=0,
        )

    def split_rows(re, im):
        re, im = finer(re), finer(im)
        left, right = [], []
        for c in range(chunks):
            piece = slice(c * half, (c + 1) * half)
            left += [re[piece], im[piece]]
            right += [-im[piece], re[piece]]
        return jnp.concatenate([jnp.concatenate(left, axis=0), jnp.concatenate(right, axis=0)], axis=1)

    def chunked_columns(x):
        return jnp.concatenate([finer(x[:lows])[:half], finer(x[lows:])[:half],
                                finer(x[:lows])[half:], finer(x[lows:])[half:]], axis=0)

    def put_low(at, re, im, finely):
        if finely:
            wide = split_rows(re, im)
        else:
            wide = jnp.concatenate(
                [jnp.concatenate([re, im], axis=0), jnp.concatenate([-im, re], axis=0)], axis=1
            )
        w_ref[at, 0], w_ref[at, 1] = parts(chunked_columns(wide.T))

    def tops_after_mids(s):
        tr, ti = gate(s, 2)
        left = parts(
            jnp.concatenate(
                [jnp.concatenate([tr, -ti], axis=1), jnp.concatenate([ti, tr], axis=1)], axis=0
            )
        )
        zero = jnp.zeros((upper, order), jnp.float32)
        for t in range(rest):
            blocks = []
            for ref in (gr_ref, gi_ref):
                mid = ref[s // 4, s % 4, 1, pl.ds(t, upper, stride=rest), :]
                for h in range(high):
                    blocks.append(jnp.concatenate([mid if g == h else zero for g in range(high)], axis=1))
            out = dot(left, parts(jnp.concatenate(blocks, axis=0)))
            for c in range(2):
                for h in range(high):
                    for g in range(high):
                        kf_ref[c, g, h, pl.ds(t, upper, stride=rest), :] = out[
                            c * order + h * upper : c * order + (h + 1) * upper, g * order : (g + 1) * order
                        ]
        return tuple(
            jnp.concatenate([kf_ref[c, g].reshape(rows, order) for g in range(high)], axis=1) for c in range(2)
        )

    def put_high(at, pair):
        km_ref[at, 0], km_ref[at, 1] = parts(jnp.concatenate(pair, axis=0))

    def high_of(at):
        return km_ref[at, 0], km_ref[at, 1]

    lane = lax.broadcasted_iota(jnp.int32, (rows, lows), 1)
    sign = jnp.where(lane < half, -1.0, 1.0)

    def apply(at, x):
        out = dot(high_of(at), parts(x))
        return out[:rows] + sign * pltpu.roll(out[rows:], half, 1)

    first[0].wait()
    first[1].wait()
    low = parts(split_rows(*product((lr_ref[1], li_ref[1]), (lr_ref[0], li_ref[0]))))
    first[2].wait()
    first[3].wait()
    state = jnp.concatenate([st_ref[0], st_ref[1]], axis=1)
    state = dot(parts(state), low, ((1,), (1,)))
    for c in range(chunks):
        sends[0][c] = state[:, c * lows : (c + 1) * lows].reshape(nfar, rows // nfar, lows)
    pl.semaphore_wait(barrier, nfar - 1 + nnear - 1)
    for c in range(chunks):
        launch(0, c)

    for load in others:
        load.wait()
    put_high(0, tops_after_mids(0))
    put_high(1, tops_after_mids(2))
    k1 = tops_after_mids(1)
    out = dot(high_of(1), parts(jnp.concatenate(k1, axis=1)))
    put_high(1, (out[:rows, :rows] - out[rows:, rows:], out[rows:, :rows] + out[:rows, rows:]))
    put_high(2, tops_after_mids(3))

    count = order // nnear
    for c in range(chunks):
        arrive(0, c)
        x = apply(0, recvs[0][c].reshape(rows, lows))
        for b in range(nnear):
            for h in range(high):
                sends[1][c, b, h] = x[h * order + b * count : h * order + (b + 1) * count]
        launch(1, c)
        if c == 0:
            put_high(3, tops_after_mids(4))

    for c in range(chunks):
        arrive(1, c)
        x = jnp.concatenate([recvs[1][c, :, h].reshape(order, lows) for h in range(high)], axis=0)
        x = trade(apply(1, x), rows // 2, half // 2, 3)
        sends[2][c] = apply(2, x).reshape(nfar, rows // nfar, lows)
        launch(2, c)

    put_high(4, tops_after_mids(6))
    k5 = tops_after_mids(5)
    out = dot(high_of(4), parts(jnp.concatenate(k5, axis=1)))
    put_high(4, (out[:rows, :rows] - out[rows:, rows:], out[rows:, :rows] + out[:rows, rows:]))
    put_low(0, *product(gate(5, 0), product(gate(4, 0), product(gate(3, 0), gate(2, 0)))), True)

    for c in range(chunks):
        arrive(2, c)
        x = apply(3, recvs[2][c].reshape(rows, lows))
        x = trade(x, rows // 4, half // 2, 3)
        sends[3][c] = apply(4, x).reshape(nnear, rows // nnear, lows)
        launch(3, c)

    put_high(5, tops_after_mids(7))
    put_low(1, *product(gate(7, 0), gate(6, 0)), False)

    begun = []
    for c in range(chunks):
        arrive(3, c)
        x = trade(recvs[3][c].reshape(rows, lows), rows // 2, half // 2, 3)
        piece = slice(c * lows, (c + 1) * lows)
        begun.append(dot(parts(x), (w_ref[0, 0, piece], w_ref[0, 1, piece])))
    x = begun[0] + begun[1]
    x = jnp.concatenate([trade(x[:, c * lows : (c + 1) * lows], rows // 2, half // 2, 3) for c in range(chunks)], axis=1)
    x = dot(parts(x), (w_ref[1, 0], w_ref[1, 1]))
    out = dot(high_of(5), parts(x))
    or_ref[...] = out[:rows, :lows] - out[rows:, lows:]
    oi_ref[...] = out[rows:, :lows] + out[:rows, lows:]
    for stage in range(4):
        sent = sends[stage].at[:, pl.ds(0, (nfar if stage % 2 == 0 else nnear) - 1)]
        pltpu.make_async_copy(sent, sent, send_sem.at[stage]).wait()


def one_kernel(nfar, nnear, state_real, state_imag, gate_real, gate_imag):
    shape = state_real.shape
    high, order, lows = shape[2:]
    rows = high * order
    blocks = (
        (2, nfar, rows // nfar, lows),
        (2, nnear, high, order // nnear, lows),
        (2, nfar, rows // nfar, lows),
        (2, nnear, rows // nnear, lows),
    )
    buffers = [pltpu.VMEM(block, jnp.float32) for block in blocks]
    vmem = pl.BlockSpec(memory_space=pltpu.VMEM)
    anywhere = pl.BlockSpec(memory_space=pl.ANY)
    result = pltpu.VMEM((rows, lows), jnp.float32)
    real, imag = pl.pallas_call(
        functools.partial(kernel, (nfar, nnear, high, order, lows)),
        out_shape=(result, result),
        in_specs=[anywhere] * 4,
        out_specs=(vmem, vmem),
        scratch_shapes=[
            pltpu.VMEM((2, rows, lows), jnp.float32),
            pltpu.VMEM((2, order, order), jnp.float32),
            pltpu.VMEM((2, order, order), jnp.float32),
            pltpu.VMEM(gate_real.shape, jnp.float32),
            pltpu.VMEM(gate_imag.shape, jnp.float32),
            pltpu.VMEM((2, high, high, order, order), jnp.float32),
            pltpu.VMEM((6, 2, 2 * rows, rows), jnp.bfloat16),
            pltpu.VMEM((2, 2, 2 * lows, 2 * lows), jnp.bfloat16),
        ]
        + buffers
        + buffers
        + [
            pltpu.SemaphoreType.DMA((4,)),
            pltpu.SemaphoreType.DMA((4, 2)),
            pltpu.SemaphoreType.DMA((6,)),
        ],
        compiler_params=pltpu.CompilerParams(collective_id=0, has_side_effects=True),
    )(
        state_real.reshape(rows, lows),
        state_imag.reshape(rows, lows),
        gate_real,
        gate_imag,
    )
    return real.reshape(shape), imag.reshape(shape)


def solution(mesh):
    nfar, nnear = mesh.shape["far"], mesh.shape["near"]

    def body(state_real, state_imag, gate_real, gate_imag):
        high, order, lows = state_real.shape[2:]
        fits = nfar == high * high and nnear == high * nfar and order == lows and gate_real.shape[0] == 2
        fits = fits and high == 2 and lows // nnear // 2 == 8
        if not fits:
            return on_device(state_real, state_imag, gate_real, gate_imag)
        return one_kernel(nfar, nnear, state_real, state_imag, gate_real, gate_imag)

    return jax.shard_map(
        body,
        mesh=mesh,
        in_specs=(P("far", "near", None, None, None), P("far", "near", None, None, None), P(), P()),
        out_specs=(P("far", "near", None, None, None), P("far", "near", None, None, None)),
        check_vma=False,
    )
```

```python
import functools

import jax
import jax.numpy as jnp
from jax import lax
from jax.experimental import pallas as pl
from jax.experimental.pallas import tpu as pltpu
from jax.sharding import PartitionSpec as P


def gate_low(x, g):
    return jnp.einsum(
        "...l,jl->...j", x, g, precision=lax.Precision.HIGHEST, preferred_element_type=jnp.float32
    )


def gate_mid(x, g):
    return jnp.einsum(
        "...ml,jm->...jl", x, g, precision=lax.Precision.HIGHEST, preferred_element_type=jnp.float32
    )


def gate_top(x, g):
    high, width, lows = (x.shape[-3], x.shape[-2], x.shape[-1])
    upper = g.shape[0] // high
    lead = x.shape[:-3]
    viewed = x.reshape(lead + (high, upper, width // upper, lows))
    matrix = g.reshape((g.shape[0], high, upper))
    out = jnp.einsum(
        "...hkrl,jhk->...jrl",
        viewed,
        matrix,
        precision=lax.Precision.HIGHEST,
        preferred_element_type=jnp.float32,
    )
    return out.reshape(lead + (high, width, lows))


def complex_gate(form, real, imag, greal, gimag):
    new_real = form(real, greal) - form(imag, gimag)
    new_imag = form(imag, greal) + form(real, gimag)
    return (new_real, new_imag)


def merged_rows(x):
    return x.reshape((1, 1, x.shape[2] * x.shape[3], x.shape[4]))


def on_device(state_real, state_imag, gate_real, gate_imag):
    real, imag = (state_real, state_imag)
    forms = (gate_low, gate_mid, gate_top)
    shape = state_real.shape
    for rnd in range(gate_real.shape[0]):
        for section in range(4):
            if section == 2:
                order = [1, 0, 2]
            else:
                order = [0, 1, 2]
            early = []
            later = order[len(early) :]
            pair = (real, imag)
            if section == 0:
                moved = (
                    lax.all_to_all(
                        merged_rows(pair[0]), "far", split_axis=2, concat_axis=2, tiled=True
                    ),
                    lax.all_to_all(
                        merged_rows(pair[1]), "far", split_axis=2, concat_axis=2, tiled=True
                    ),
                )
                pair = (moved[0].reshape(shape), moved[1].reshape(shape))
            elif section == 1:
                pair = (
                    lax.all_to_all(pair[0], "near", split_axis=3, concat_axis=3, tiled=True),
                    lax.all_to_all(pair[1], "near", split_axis=3, concat_axis=3, tiled=True),
                )
            elif section == 2:
                pair = (
                    lax.all_to_all(pair[0], "near", split_axis=4, concat_axis=4, tiled=True),
                    lax.all_to_all(pair[1], "near", split_axis=4, concat_axis=4, tiled=True),
                )
            else:
                moved = (
                    lax.all_to_all(
                        merged_rows(pair[0]), "near", split_axis=2, concat_axis=2, tiled=True
                    ),
                    lax.all_to_all(
                        merged_rows(pair[1]), "near", split_axis=2, concat_axis=2, tiled=True
                    ),
                )
                pair = (moved[0].reshape(shape), moved[1].reshape(shape))
            for which in later:
                pair = complex_gate(
                    forms[which],
                    pair[0],
                    pair[1],
                    gate_real[rnd, section, which],
                    gate_imag[rnd, section, which],
                )
            real, imag = pair
    return (real, imag)


def parts(x):
    first = x.astype(jnp.bfloat16)
    return first, (x - first.astype(jnp.float32)).astype(jnp.bfloat16)


def dot(a, b, dims=((1,), (0,))):
    def product(x, y):
        return lax.dot_general(x, y, (dims, ((), ())), preferred_element_type=jnp.float32)

    return product(a[0], b[0]) + (product(a[0], b[1]) + product(a[1], b[0]))


def complex_rows(stacked, pair):
    out = dot(stacked, parts(jnp.concatenate(pair, axis=1)))
    n, w = out.shape[0] // 2, out.shape[1] // 2
    return out[:n, :w] - out[n:, w:], out[n:, :w] + out[:n, w:]


def product(a, b):
    return complex_rows(parts(jnp.concatenate(a, axis=0)), b)


def complex_matrix(re, im):
    return jnp.concatenate(
        [jnp.concatenate([re, -im], axis=1), jnp.concatenate([im, re], axis=1)], axis=0
    )


def trade(x, swaps):
    unit = 8
    rows, lanes = x.shape
    at = lax.broadcasted_iota(jnp.int32, (unit, lanes), 1)
    steps = []
    for row, lane in swaps:
        low = lax.rem(lax.div(at, lane), 2) == 0
        steps.append((row // unit, low, jnp.where(low, at + lane, at - lane)))
    out = [None] * (rows // unit)
    for base in range(rows // unit):
        if any(base // stride % 2 for stride, _, _ in steps):
            continue
        group = [base]
        for stride, _, _ in steps:
            group = group + [i + stride for i in group]
        for i in group:
            out[i] = x[i * unit : (i + 1) * unit]
        for stride, low, other in steps:
            for i in group:
                if i // stride % 2 == 0:
                    a, b = out[i], out[i + stride]
                    moved = jnp.take_along_axis(jnp.where(low, b, a), other, axis=1)
                    out[i], out[i + stride] = jnp.where(low, a, moved), jnp.where(low, moved, b)
    return jnp.concatenate(out, axis=0)


def kernel(sizes, sr_hbm, si_hbm, gr_hbm, gi_hbm, or_ref, oi_ref, *scratch):
    nfar, nnear, high, order, lows = sizes
    (
        st_ref, lr_ref, li_ref, gr_ref, gi_ref, kf_ref, km_ref, w_ref,
        send0, send1, send2, recv0, recv1, recv2,
        send_sem, recv_sem, load_sem,
    ) = scratch
    far, near = lax.axis_index("far"), lax.axis_index("near")
    core, side = near % 2, far // 2
    upper = order // high
    rest = order // upper
    rows = high * order
    fine = lows // nnear
    eight = fine // 2

    def flips(at, bits):
        found = []
        for mask in range(2**bits):
            found.append(sum((at // 2**i % 2 + mask // 2**i % 2) % 2 * 2**i for i in range(bits)))
        return found

    fars, nears = flips(far, 2), flips(near, 3)
    others = [(a, b) for a in range(nfar) for b in range(nnear) if a + b]
    others.sort(key=lambda ab: -(ab[0] + ab[1] // 4 + ab[1] // 2 % 2))

    barrier = pltpu.get_barrier_semaphore()
    for a, b in others:
        pl.semaphore_signal(
            barrier, inc=1, device_id=(fars[a], nears[b]), device_id_type=pl.DeviceIdType.MESH
        )
    first = [
        pltpu.make_async_copy(gr_hbm.at[0, pl.ds(0, 2), 0], lr_ref, load_sem.at[0]),
        pltpu.make_async_copy(gi_hbm.at[0, pl.ds(0, 2), 0], li_ref, load_sem.at[1]),
        pltpu.make_async_copy(sr_hbm, st_ref.at[0], load_sem.at[2]),
        pltpu.make_async_copy(si_hbm, st_ref.at[1], load_sem.at[3]),
    ]
    gates = [
        pltpu.make_async_copy(gr_hbm, gr_ref, load_sem.at[4]),
        pltpu.make_async_copy(gi_hbm, gi_ref, load_sem.at[5]),
    ]
    for load in first + gates:
        load.start()

    def remote(stage, source, target, to):
        return pltpu.make_async_remote_copy(
            src_ref=source,
            dst_ref=target,
            send_sem=send_sem.at[stage],
            recv_sem=recv_sem.at[stage],
            device_id=to,
            device_id_type=pl.DeviceIdType.MESH,
        )

    def settle(ref, sem):
        pltpu.make_async_copy(ref, ref, sem).wait()

    def gate(s, which):
        return gr_ref[s // 4, s % 4, which], gi_ref[s // 4, s % 4, which]

    def tops_after_mids(s):
        left = parts(complex_matrix(*gate(s, 2)))
        zero = jnp.zeros((upper, order), jnp.float32)
        for t in range(rest):
            blocks = []
            for ref in (gr_ref, gi_ref):
                mid = ref[s // 4, s % 4, 1, pl.ds(t, upper, stride=rest), :]
                for h in range(high):
                    blocks.append(jnp.concatenate([mid if g == h else zero for g in range(high)], axis=1))
            out = dot(left, parts(jnp.concatenate(blocks, axis=0)))
            for c in range(2):
                for h in range(high):
                    for g in range(high):
                        kf_ref[c, g, h, pl.ds(t, upper, stride=rest), :] = out[
                            c * order + h * upper : c * order + (h + 1) * upper, g * order : (g + 1) * order
                        ]
        return tuple(
            jnp.concatenate([kf_ref[c, g].reshape(rows, order) for g in range(high)], axis=1) for c in range(2)
        )

    def put_high(at, pair):
        km_ref[at, 0], km_ref[at, 1] = parts(jnp.concatenate(pair, axis=0))

    def high_of(at):
        return km_ref[at, 0], km_ref[at, 1]

    def put_low(at, pair, finely):
        wide = complex_matrix(*pair).T
        if finely:
            wide = jnp.concatenate(
                [
                    wide[((c * nnear + b) * 2 + k) * eight : ((c * nnear + b) * 2 + k + 1) * eight]
                    for c in range(2)
                    for k in range(2)
                    for b in range(nnear)
                ],
                axis=0,
            )
        w_ref[at, 0], w_ref[at, 1] = parts(wide)

    def low_gate(at, pair):
        out = dot(parts(jnp.concatenate(pair, axis=1)), (w_ref[at, 0], w_ref[at, 1]))
        return out[:, :lows], out[:, lows:]

    def traded(pair, swaps):
        return tuple(trade(x, swaps) for x in pair)

    first[0].wait()
    first[1].wait()
    last = tuple(
        jnp.concatenate([ref[1, pl.ds(k, nnear, stride=fine), :] for k in range(fine)], axis=0)
        for ref in (lr_ref, li_ref)
    )
    low = parts(complex_matrix(*product(last, (lr_ref[0], li_ref[0]))))
    first[2].wait()
    first[3].wait()
    state = dot(parts(jnp.concatenate([st_ref[0], st_ref[1]], axis=1)), low, ((1,), (1,)))
    pair = traded((state[:, :lows], state[:, lows:]), ((64, 64), (32, 32), (16, 16), (8, 8)))
    for c in range(2):
        for h in range(high):
            for k in range(fine):
                at = (h * fine + k) * eight
                send0[k * high + h, c] = pair[c][at : at + eight]
    pl.semaphore_wait(barrier, nfar * nnear - 1)
    me = far * nnear + near
    for a, b in others:
        remote(0, send0.at[fars[a] * nnear + nears[b]], recv0.at[me], (fars[a], nears[b])).start()
    recv0[me] = send0[me]

    for load in gates:
        load.wait()
    put_high(0, tops_after_mids(0))
    put_high(1, tops_after_mids(2))
    put_high(1, complex_rows(high_of(1), tops_after_mids(1)))
    put_high(2, tops_after_mids(3))
    put_high(3, tops_after_mids(4))
    put_high(4, tops_after_mids(6))
    put_high(4, complex_rows(high_of(4), tops_after_mids(5)))

    settle(recv0.at[pl.ds(0, nfar * nnear - 1)], recv_sem.at[0])
    pair = tuple(recv0[:, c].reshape(rows, lows) for c in range(2))
    pair = complex_rows(high_of(0), traded(pair, ((32, 32), (16, 16), (8, 8))))
    pair = complex_rows(high_of(1), traded(pair, ((64, 32), (32, 16), (16, 8))))
    pair = complex_rows(high_of(2), traded(pair, ((128, 4), (64, 2), (32, 1))))
    for c in range(2):
        for k in range(2):
            send1[k, c] = pair[c][k * order : (k + 1) * order]
    remote(1, send1.at[1 - core], recv1.at[core], (far, nears[1])).start()
    recv1[core] = send1[core]
    settle(recv1.at[0], recv_sem.at[1])

    pair = tuple(recv1[:, c].reshape(rows, lows) for c in range(2))
    pair = complex_rows(high_of(3), traded(pair, ((64, 64),)))
    pair = complex_rows(high_of(4), traded(pair, ((64, 4), (32, 2), (16, 1))))
    pair = traded(pair, ((16, 64),))
    thin = rows // nnear // 2
    for c in range(2):
        for b in range(nnear):
            for k in range(2):
                at = (b * 2 + k) * thin
                send2[k * nnear + b, c] = pair[c][at : at + thin]
    here = far * (nnear // 2) + near // 2
    same = side == core
    for b in (6, 7, 4, 5, 2, 3, 1, 0):
        for a in (1, 0):
            to = (core * 2 + (far % 2 + a) % 2, nears[b])
            copy = remote(2, send2.at[to[0] % 2 * nnear + to[1]], recv2.at[here], to)
            if a + b:
                copy.start()
            else:
                @pl.when(jnp.logical_not(same))
                def _():
                    copy.start()

                @pl.when(same)
                def _():
                    recv2[here] = send2[far % 2 * nnear + near]

    put_high(5, tops_after_mids(7))
    put_low(0, product(gate(5, 0), product(gate(4, 0), product(gate(3, 0), gate(2, 0)))), True)
    put_low(1, product(gate(7, 0), gate(6, 0)), False)

    count = 2 * nnear

    @pl.when(same)
    def _():
        settle(recv2.at[pl.ds(0, count - 1)], recv_sem.at[2])

    @pl.when(jnp.logical_not(same))
    def _():
        settle(recv2, recv_sem.at[2])

    pair = tuple(recv2[:, c].reshape(rows, lows) for c in range(2))
    pair = low_gate(0, traded(pair, ((128, 64), (64, 4), (32, 2), (16, 1))))
    pair = low_gate(1, traded(pair, ((64, 64), (32, 32), (16, 16))))
    pair = tuple(
        jnp.concatenate(
            [x[(k * nnear + b) * thin : (k * nnear + b + 1) * thin] for b in range(nnear) for k in range(2)], axis=0
        )
        for x in pair
    )
    or_ref[...], oi_ref[...] = complex_rows(high_of(5), pair)

    settle(send0.at[pl.ds(0, nfar * nnear - 1)], send_sem.at[0])
    settle(send1.at[0], send_sem.at[1])

    @pl.when(same)
    def _():
        settle(send2.at[pl.ds(0, count - 1)], send_sem.at[2])

    @pl.when(jnp.logical_not(same))
    def _():
        settle(send2, send_sem.at[2])


def one_kernel(nfar, nnear, state_real, state_imag, gate_real, gate_imag):
    shape = state_real.shape
    high, order, lows = shape[2:]
    rows = high * order
    blocks = (
        (nfar * nnear, 2, rows // nfar // nnear, lows),
        (2, 2, rows // 2, lows),
        (2 * nnear, 2, rows // nnear // 2, lows),
    )
    buffers = [pltpu.VMEM(block, jnp.float32) for block in blocks]
    vmem = pl.BlockSpec(memory_space=pltpu.VMEM)
    anywhere = pl.BlockSpec(memory_space=pl.ANY)
    result = pltpu.VMEM((rows, lows), jnp.float32)
    real, imag = pl.pallas_call(
        functools.partial(kernel, (nfar, nnear, high, order, lows)),
        out_shape=(result, result),
        in_specs=[anywhere] * 4,
        out_specs=(vmem, vmem),
        scratch_shapes=[
            pltpu.VMEM((2, rows, lows), jnp.float32),
            pltpu.VMEM((2, order, order), jnp.float32),
            pltpu.VMEM((2, order, order), jnp.float32),
            pltpu.VMEM(gate_real.shape, jnp.float32),
            pltpu.VMEM(gate_imag.shape, jnp.float32),
            pltpu.VMEM((2, high, high, order, order), jnp.float32),
            pltpu.VMEM((6, 2, 2 * rows, rows), jnp.bfloat16),
            pltpu.VMEM((2, 2, 2 * lows, 2 * lows), jnp.bfloat16),
        ]
        + buffers
        + buffers
        + [
            pltpu.SemaphoreType.DMA((3,)),
            pltpu.SemaphoreType.DMA((3,)),
            pltpu.SemaphoreType.DMA((6,)),
        ],
        compiler_params=pltpu.CompilerParams(collective_id=0, has_side_effects=True),
    )(
        state_real.reshape(rows, lows),
        state_imag.reshape(rows, lows),
        gate_real,
        gate_imag,
    )
    return real.reshape(shape), imag.reshape(shape)


def solution(mesh):
    nfar, nnear = mesh.shape["far"], mesh.shape["near"]

    def body(state_real, state_imag, gate_real, gate_imag):
        high, order, lows = state_real.shape[2:]
        fits = high == 2 and nfar == high**2 and nnear == high**3 and order == lows and gate_real.shape[0] == 2
        fits = fits and lows == 2 * nnear * 8
        if not fits:
            return on_device(state_real, state_imag, gate_real, gate_imag)
        return one_kernel(nfar, nnear, state_real, state_imag, gate_real, gate_imag)

    return jax.shard_map(
        body,
        mesh=mesh,
        in_specs=(P("far", "near", None, None, None), P("far", "near", None, None, None), P(), P()),
        out_specs=(P("far", "near", None, None, None), P("far", "near", None, None, None)),
        check_vma=False,
    )
```

```python
import functools

import jax
import jax.numpy as jnp
from jax import lax
from jax.experimental import pallas as pl
from jax.experimental.pallas import tpu as pltpu
from jax.sharding import PartitionSpec as P


def gate_low(x, g):
    return jnp.einsum(
        "...l,jl->...j", x, g, precision=lax.Precision.HIGHEST, preferred_element_type=jnp.float32
    )


def gate_mid(x, g):
    return jnp.einsum(
        "...ml,jm->...jl", x, g, precision=lax.Precision.HIGHEST, preferred_element_type=jnp.float32
    )


def gate_top(x, g):
    high, width, lows = (x.shape[-3], x.shape[-2], x.shape[-1])
    upper = g.shape[0] // high
    lead = x.shape[:-3]
    viewed = x.reshape(lead + (high, upper, width // upper, lows))
    matrix = g.reshape((g.shape[0], high, upper))
    out = jnp.einsum(
        "...hkrl,jhk->...jrl",
        viewed,
        matrix,
        precision=lax.Precision.HIGHEST,
        preferred_element_type=jnp.float32,
    )
    return out.reshape(lead + (high, width, lows))


def complex_gate(form, real, imag, greal, gimag):
    new_real = form(real, greal) - form(imag, gimag)
    new_imag = form(imag, greal) + form(real, gimag)
    return (new_real, new_imag)


def merged_rows(x):
    return x.reshape((1, 1, x.shape[2] * x.shape[3], x.shape[4]))


def on_device(state_real, state_imag, gate_real, gate_imag):
    real, imag = (state_real, state_imag)
    forms = (gate_low, gate_mid, gate_top)
    shape = state_real.shape
    for rnd in range(gate_real.shape[0]):
        for section in range(4):
            if section == 2:
                order = [1, 0, 2]
            else:
                order = [0, 1, 2]
            early = []
            later = order[len(early) :]
            pair = (real, imag)
            if section == 0:
                moved = (
                    lax.all_to_all(
                        merged_rows(pair[0]), "far", split_axis=2, concat_axis=2, tiled=True
                    ),
                    lax.all_to_all(
                        merged_rows(pair[1]), "far", split_axis=2, concat_axis=2, tiled=True
                    ),
                )
                pair = (moved[0].reshape(shape), moved[1].reshape(shape))
            elif section == 1:
                pair = (
                    lax.all_to_all(pair[0], "near", split_axis=3, concat_axis=3, tiled=True),
                    lax.all_to_all(pair[1], "near", split_axis=3, concat_axis=3, tiled=True),
                )
            elif section == 2:
                pair = (
                    lax.all_to_all(pair[0], "near", split_axis=4, concat_axis=4, tiled=True),
                    lax.all_to_all(pair[1], "near", split_axis=4, concat_axis=4, tiled=True),
                )
            else:
                moved = (
                    lax.all_to_all(
                        merged_rows(pair[0]), "near", split_axis=2, concat_axis=2, tiled=True
                    ),
                    lax.all_to_all(
                        merged_rows(pair[1]), "near", split_axis=2, concat_axis=2, tiled=True
                    ),
                )
                pair = (moved[0].reshape(shape), moved[1].reshape(shape))
            for which in later:
                pair = complex_gate(
                    forms[which],
                    pair[0],
                    pair[1],
                    gate_real[rnd, section, which],
                    gate_imag[rnd, section, which],
                )
            real, imag = pair
    return (real, imag)


def parts(x):
    first = x.astype(jnp.bfloat16)
    return first, (x - first.astype(jnp.float32)).astype(jnp.bfloat16)


def dot(a, b, dims=((1,), (0,))):
    def product(x, y):
        return lax.dot_general(x, y, (dims, ((), ())), preferred_element_type=jnp.float32)

    return product(a[0], b[0]) + (product(a[0], b[1]) + product(a[1], b[0]))


def split(pair):
    return parts(jnp.concatenate(pair, axis=1))


def complex_rows(stacked, pair):
    out = dot(stacked, pair)
    n, w = out.shape[0] // 2, out.shape[1] // 2
    return out[:n, :w] - out[n:, w:], out[n:, :w] + out[:n, w:]


def product(a, b):
    return complex_rows(parts(jnp.concatenate(a, axis=0)), split(b))


def complex_matrix(re, im):
    return jnp.concatenate(
        [jnp.concatenate([re, -im], axis=1), jnp.concatenate([im, re], axis=1)], axis=0
    )


def trade(x, swaps):
    unit = 8
    rows, lanes = x.shape
    at = lax.broadcasted_iota(jnp.int32, (unit, lanes), 1)
    steps = []
    for row, lane in swaps:
        low = lax.rem(lax.div(at, lane), 2) == 0
        steps.append((row // unit, low, jnp.where(low, at + lane, at - lane)))
    out = [None] * (rows // unit)
    for base in range(rows // unit):
        if any(base // stride % 2 for stride, _, _ in steps):
            continue
        group = [base]
        for stride, _, _ in steps:
            group = group + [i + stride for i in group]
        for i in group:
            out[i] = x[i * unit : (i + 1) * unit]
        for stride, low, other in steps:
            for i in group:
                if i // stride % 2 == 0:
                    a, b = out[i], out[i + stride]
                    moved = jnp.take_along_axis(jnp.where(low, b, a), other, axis=1)
                    out[i], out[i + stride] = jnp.where(low, a, moved), jnp.where(low, moved, b)
    return jnp.concatenate(out, axis=0)


def kernel(sizes, sr_hbm, si_hbm, gr_hbm, gi_hbm, o_ref, *scratch):
    nfar, nnear, high, order, lows = sizes
    (
        st_ref, lr_ref, li_ref, gr_ref, gi_ref, kf_ref, km_ref, w_ref,
        send0, send1, send2, recv0, recv1, recv2,
        x_ref, send_sem, recv_sem, load_sem,
    ) = scratch
    far, near = lax.axis_index("far"), lax.axis_index("near")
    core, side = near % 2, far // 2
    upper = order // high
    rest = order // upper
    rows = high * order
    fine = lows // nnear
    eight = fine // 2

    def flips(at, bits):
        found = []
        for mask in range(2**bits):
            found.append(sum((at // 2**i % 2 + mask // 2**i % 2) % 2 * 2**i for i in range(bits)))
        return found

    fars, nears = flips(far, 2), flips(near, 3)
    others = [(a, b) for a in range(nfar) for b in range(nnear) if a + b]
    others.sort(key=lambda ab: -(ab[0] + ab[1] // 4 + ab[1] // 2 % 2))

    barrier = pltpu.get_barrier_semaphore()
    for a, b in others:
        pl.semaphore_signal(
            barrier, inc=1, device_id=(fars[a], nears[b]), device_id_type=pl.DeviceIdType.MESH
        )
    first = [
        pltpu.make_async_copy(gr_hbm.at[0, pl.ds(0, 2), 0], lr_ref, load_sem.at[0]),
        pltpu.make_async_copy(gi_hbm.at[0, pl.ds(0, 2), 0], li_ref, load_sem.at[1]),
        pltpu.make_async_copy(sr_hbm, st_ref.at[0], load_sem.at[2]),
        pltpu.make_async_copy(si_hbm, st_ref.at[1], load_sem.at[3]),
    ]
    gates = [
        pltpu.make_async_copy(gr_hbm, gr_ref, load_sem.at[4]),
        pltpu.make_async_copy(gi_hbm, gi_ref, load_sem.at[5]),
    ]
    for load in first + gates:
        load.start()

    def remote(stage, source, target, to, group=0):
        return pltpu.make_async_remote_copy(
            src_ref=source,
            dst_ref=target,
            send_sem=send_sem.at[stage],
            recv_sem=recv_sem.at[stage + group],
            device_id=to,
            device_id_type=pl.DeviceIdType.MESH,
        )

    def settle(ref, sem):
        pltpu.make_async_copy(ref, ref, sem).wait()

    def gate(s, which):
        return gr_ref[s // 4, s % 4, which], gi_ref[s // 4, s % 4, which]

    def tops_after_mids(s):
        left = parts(complex_matrix(*gate(s, 2)))
        zero = jnp.zeros((upper, order), jnp.float32)
        for t in range(rest):
            blocks = []
            for ref in (gr_ref, gi_ref):
                mid = ref[s // 4, s % 4, 1, pl.ds(t, upper, stride=rest), :]
                for h in range(high):
                    blocks.append(jnp.concatenate([mid if g == h else zero for g in range(high)], axis=1))
            out = dot(left, parts(jnp.concatenate(blocks, axis=0)))
            for c in range(2):
                for h in range(high):
                    for g in range(high):
                        kf_ref[c, g, h, pl.ds(t, upper, stride=rest), :] = out[
                            c * order + h * upper : c * order + (h + 1) * upper, g * order : (g + 1) * order
                        ]
        return tuple(
            jnp.concatenate([kf_ref[c, g].reshape(rows, order) for g in range(high)], axis=1) for c in range(2)
        )

    def put_high(at, pair):
        km_ref[at, 0], km_ref[at, 1] = parts(jnp.concatenate(pair, axis=0))

    def high_of(at):
        return km_ref[at, 0], km_ref[at, 1]

    def rows_of(at, half):
        places = [pl.ds(pl.multiple_of(half * order, order) + c * rows, order) for c in range(2)]
        return tuple(jnp.concatenate([km_ref[at, p, place] for place in places], axis=0) for p in range(2))

    def put_low(at, pair, finely):
        wide = complex_matrix(*pair).T
        if finely:
            wide = jnp.concatenate(
                [
                    wide[((c * nnear + b) * 2 + k) * eight : ((c * nnear + b) * 2 + k + 1) * eight]
                    for c in range(2)
                    for k in range(2)
                    for b in range(nnear)
                ],
                axis=0,
            )
        w_ref[at, 0], w_ref[at, 1] = parts(wide)

    def low_gate(at, pair):
        out = dot(parts(jnp.concatenate(pair, axis=1)), (w_ref[at, 0], w_ref[at, 1]))
        return out[:, :lows], out[:, lows:]

    def traded(pair, swaps):
        return tuple(trade(x, swaps) for x in pair)

    first[0].wait()
    first[1].wait()
    last = tuple(
        jnp.concatenate([ref[1, pl.ds(k, nnear, stride=fine), :] for k in range(fine)], axis=0)
        for ref in (lr_ref, li_ref)
    )
    low = parts(complex_matrix(*product(last, (lr_ref[0], li_ref[0]))))
    first[2].wait()
    first[3].wait()
    state = dot(parts(jnp.concatenate([st_ref[0], st_ref[1]], axis=1)), low, ((1,), (1,)))
    pair = traded((state[:, :lows], state[:, lows:]), ((64, 64), (32, 32), (16, 16), (8, 8)))
    for c in range(2):
        for h in range(high):
            for k in range(fine):
                at = (h * fine + k) * eight
                send0[k * high + h, c] = pair[c][at : at + eight]
    pl.semaphore_wait(barrier, nfar * nnear - 1)
    me = far * nnear + near
    for a, b in others:
        remote(0, send0.at[fars[a] * nnear + nears[b]], recv0.at[me], (fars[a], nears[b]), 3 * a).start()
    recv0[me] = send0[me]

    for load in gates:
        load.wait()
    put_high(0, tops_after_mids(0))
    put_high(1, tops_after_mids(2))
    put_high(1, complex_rows(high_of(1), split(tops_after_mids(1))))
    put_high(2, tops_after_mids(3))
    put_high(3, tops_after_mids(4))
    put_high(4, tops_after_mids(6))
    put_high(4, complex_rows(high_of(4), split(tops_after_mids(5))))

    def keep(at, pair):
        count = pair[0].shape[0]
        place = pl.ds(pl.multiple_of(at * count, count), count)
        x_ref[0, place], x_ref[1, place] = parts(jnp.concatenate(pair, axis=1))

    for a in range(nfar):
        landed = recv0.at[pl.ds(fars[a] * nnear, nnear - 1 if a == 0 else nnear)]
        settle(landed, recv_sem.at[3 * a])
        pair = tuple(recv0[pl.ds(fars[a] * nnear, nnear), c].reshape(rows // nfar, lows) for c in range(2))
        keep(fars[a], traded(pair, ((32, 32), (16, 16), (8, 8))))
    pair = complex_rows(high_of(0), (x_ref[0], x_ref[1]))
    pair = complex_rows(high_of(1), split(traded(pair, ((64, 32), (32, 16), (16, 8)))))
    ready = split(traded(pair, ((128, 4), (64, 2), (32, 1))))
    send1[0], send1[1] = complex_rows(rows_of(2, 1 - core), ready)
    remote(1, send1, recv1, (far, nears[1])).start()
    keep(core, traded(complex_rows(rows_of(2, core), ready), ((64, 64),)))
    settle(recv1, recv_sem.at[1])
    keep(1 - core, traded((recv1[0], recv1[1]), ((64, 64),)))
    pair = complex_rows(high_of(3), (x_ref[0], x_ref[1]))
    ready = split(traded(pair, ((64, 4), (32, 2), (16, 1))))
    thin = rows // nnear // 2
    here = far * (nnear // 2) + near // 2
    same = side == core
    for h in (1, 0):
        top = (near // 4 + h) % 2
        pair = traded(complex_rows(rows_of(4, top), ready), ((16, 64),))
        for c in range(2):
            for b in range(nnear // 2):
                for k in range(2):
                    at = (b * 2 + k) * thin
                    send2[k * nnear + top * (nnear // 2) + b, c] = pair[c][at : at + thin]
        for b in (2, 3, 1, 0):
            for a in (1, 0):
                to = (core * 2 + (far % 2 + a) % 2, nears[4 * h + b])
                copy = remote(2, send2.at[to[0] % 2 * nnear + to[1]], recv2.at[here], to)
                if a + b + h:
                    copy.start()
                else:
                    @pl.when(jnp.logical_not(same))
                    def _():
                        copy.start()

                    @pl.when(same)
                    def _():
                        recv2[here] = send2[far % 2 * nnear + near]

    put_high(5, tops_after_mids(7))
    put_low(0, product(gate(5, 0), product(gate(4, 0), product(gate(3, 0), gate(2, 0)))), True)
    put_low(1, product(gate(7, 0), gate(6, 0)), False)

    count = 2 * nnear

    @pl.when(same)
    def _():
        settle(recv2.at[pl.ds(0, count - 1)], recv_sem.at[2])

    @pl.when(jnp.logical_not(same))
    def _():
        settle(recv2, recv_sem.at[2])

    pair = tuple(recv2[:, c].reshape(rows, lows) for c in range(2))
    pair = low_gate(0, traded(pair, ((128, 64), (64, 4), (32, 2), (16, 1))))
    pair = low_gate(1, traded(pair, ((64, 64), (32, 32), (16, 16))))
    pair = tuple(
        jnp.concatenate(
            [x[(k * nnear + b) * thin : (k * nnear + b + 1) * thin] for b in range(nnear) for k in range(2)], axis=0
        )
        for x in pair
    )
    o_ref[0], o_ref[1] = complex_rows(high_of(5), split(pair))

    settle(send0.at[pl.ds(0, nfar * nnear - 1)], send_sem.at[0])
    settle(send1, send_sem.at[1])

    @pl.when(same)
    def _():
        settle(send2.at[pl.ds(0, count - 1)], send_sem.at[2])

    @pl.when(jnp.logical_not(same))
    def _():
        settle(send2, send_sem.at[2])


def one_kernel(nfar, nnear, state_real, state_imag, gate_real, gate_imag):
    shape = state_real.shape
    high, order, lows = shape[2:]
    rows = high * order
    blocks = (
        (nfar * nnear, 2, rows // nfar // nnear, lows),
        (2, rows // 2, lows),
        (2 * nnear, 2, rows // nnear // 2, lows),
    )
    buffers = [pltpu.VMEM(block, jnp.float32) for block in blocks]
    vmem = pl.BlockSpec(memory_space=pltpu.VMEM)
    anywhere = pl.BlockSpec(memory_space=pl.ANY)
    result = pltpu.VMEM((rows, lows), jnp.float32)
    both = pl.pallas_call(
        functools.partial(kernel, (nfar, nnear, high, order, lows)),
        out_shape=pltpu.VMEM((2, rows, lows), jnp.float32),
        in_specs=[anywhere] * 4,
        out_specs=vmem,
        scratch_shapes=[
            pltpu.VMEM((2, rows, lows), jnp.float32),
            pltpu.VMEM((2, order, order), jnp.float32),
            pltpu.VMEM((2, order, order), jnp.float32),
            pltpu.VMEM(gate_real.shape, jnp.float32),
            pltpu.VMEM(gate_imag.shape, jnp.float32),
            pltpu.VMEM((2, high, high, order, order), jnp.float32),
            pltpu.VMEM((6, 2, 2 * rows, rows), jnp.bfloat16),
            pltpu.VMEM((2, 2, 2 * lows, 2 * lows), jnp.bfloat16),
        ]
        + buffers
        + buffers
        + [
            pltpu.VMEM((2, rows, 2 * lows), jnp.bfloat16),
            pltpu.SemaphoreType.DMA((3,)),
            pltpu.SemaphoreType.DMA((3 * nfar,)),
            pltpu.SemaphoreType.DMA((6,)),
        ],
        compiler_params=pltpu.CompilerParams(collective_id=0, has_side_effects=True),
    )(
        state_real.reshape(rows, lows),
        state_imag.reshape(rows, lows),
        gate_real,
        gate_imag,
    )
    return both[0].reshape(shape), both[1].reshape(shape)


def solution(mesh):
    nfar, nnear = mesh.shape["far"], mesh.shape["near"]

    def body(state_real, state_imag, gate_real, gate_imag):
        high, order, lows = state_real.shape[2:]
        fits = high == 2 and nfar == high**2 and nnear == high**3 and order == lows and gate_real.shape[0] == 2
        fits = fits and lows == 2 * nnear * 8
        if not fits:
            return on_device(state_real, state_imag, gate_real, gate_imag)
        return one_kernel(nfar, nnear, state_real, state_imag, gate_real, gate_imag)

    return jax.shard_map(
        body,
        mesh=mesh,
        in_specs=(P("far", "near", None, None, None), P("far", "near", None, None, None), P(), P()),
        out_specs=(P("far", "near", None, None, None), P("far", "near", None, None, None)),
        check_vma=False,
    )
```

```python
import functools

import jax
import jax.numpy as jnp
from jax import lax
from jax.experimental import pallas as pl
from jax.experimental.pallas import tpu as pltpu
from jax.sharding import PartitionSpec as P


def gate_low(x, g):
    return jnp.einsum(
        "...l,jl->...j", x, g, precision=lax.Precision.HIGHEST, preferred_element_type=jnp.float32
    )


def gate_mid(x, g):
    return jnp.einsum(
        "...ml,jm->...jl", x, g, precision=lax.Precision.HIGHEST, preferred_element_type=jnp.float32
    )


def gate_top(x, g):
    high, width, lows = (x.shape[-3], x.shape[-2], x.shape[-1])
    upper = g.shape[0] // high
    lead = x.shape[:-3]
    viewed = x.reshape(lead + (high, upper, width // upper, lows))
    matrix = g.reshape((g.shape[0], high, upper))
    out = jnp.einsum(
        "...hkrl,jhk->...jrl",
        viewed,
        matrix,
        precision=lax.Precision.HIGHEST,
        preferred_element_type=jnp.float32,
    )
    return out.reshape(lead + (high, width, lows))


def complex_gate(form, real, imag, greal, gimag):
    new_real = form(real, greal) - form(imag, gimag)
    new_imag = form(imag, greal) + form(real, gimag)
    return (new_real, new_imag)


def merged_rows(x):
    return x.reshape((1, 1, x.shape[2] * x.shape[3], x.shape[4]))


def on_device(state_real, state_imag, gate_real, gate_imag):
    real, imag = (state_real, state_imag)
    forms = (gate_low, gate_mid, gate_top)
    shape = state_real.shape
    for rnd in range(gate_real.shape[0]):
        for section in range(4):
            if section == 2:
                order = [1, 0, 2]
            else:
                order = [0, 1, 2]
            early = []
            later = order[len(early) :]
            pair = (real, imag)
            if section == 0:
                moved = (
                    lax.all_to_all(
                        merged_rows(pair[0]), "far", split_axis=2, concat_axis=2, tiled=True
                    ),
                    lax.all_to_all(
                        merged_rows(pair[1]), "far", split_axis=2, concat_axis=2, tiled=True
                    ),
                )
                pair = (moved[0].reshape(shape), moved[1].reshape(shape))
            elif section == 1:
                pair = (
                    lax.all_to_all(pair[0], "near", split_axis=3, concat_axis=3, tiled=True),
                    lax.all_to_all(pair[1], "near", split_axis=3, concat_axis=3, tiled=True),
                )
            elif section == 2:
                pair = (
                    lax.all_to_all(pair[0], "near", split_axis=4, concat_axis=4, tiled=True),
                    lax.all_to_all(pair[1], "near", split_axis=4, concat_axis=4, tiled=True),
                )
            else:
                moved = (
                    lax.all_to_all(
                        merged_rows(pair[0]), "near", split_axis=2, concat_axis=2, tiled=True
                    ),
                    lax.all_to_all(
                        merged_rows(pair[1]), "near", split_axis=2, concat_axis=2, tiled=True
                    ),
                )
                pair = (moved[0].reshape(shape), moved[1].reshape(shape))
            for which in later:
                pair = complex_gate(
                    forms[which],
                    pair[0],
                    pair[1],
                    gate_real[rnd, section, which],
                    gate_imag[rnd, section, which],
                )
            real, imag = pair
    return (real, imag)


def parts(x):
    first = x.astype(jnp.bfloat16)
    return first, (x - first.astype(jnp.float32)).astype(jnp.bfloat16)


def dot(a, b, dims=((1,), (0,))):
    def product(x, y):
        return lax.dot_general(x, y, (dims, ((), ())), preferred_element_type=jnp.float32)

    return product(a[0], b[0]) + (product(a[0], b[1]) + product(a[1], b[0]))


def split(pair):
    return parts(jnp.concatenate(pair, axis=1))


def complex_rows(stacked, pair):
    out = dot(stacked, pair)
    n, w = out.shape[0] // 2, out.shape[1] // 2
    return out[:n, :w] - out[n:, w:], out[n:, :w] + out[:n, w:]


def product(a, b):
    return complex_rows(parts(jnp.concatenate(a, axis=0)), split(b))


def complex_matrix(re, im):
    return jnp.concatenate(
        [jnp.concatenate([re, -im], axis=1), jnp.concatenate([im, re], axis=1)], axis=0
    )


def trade(x, swaps):
    unit = 8
    rows, lanes = x.shape
    at = lax.broadcasted_iota(jnp.int32, (unit, lanes), 1)
    steps = []
    for row, lane in swaps:
        low = lax.rem(lax.div(at, lane), 2) == 0
        steps.append((row // unit, low, jnp.where(low, at + lane, at - lane)))
    out = [None] * (rows // unit)
    for base in range(rows // unit):
        if any(base // stride % 2 for stride, _, _ in steps):
            continue
        group = [base]
        for stride, _, _ in steps:
            group = group + [i + stride for i in group]
        for i in group:
            out[i] = x[i * unit : (i + 1) * unit]
        for stride, low, other in steps:
            for i in group:
                if i // stride % 2 == 0:
                    a, b = out[i], out[i + stride]
                    moved = jnp.take_along_axis(jnp.where(low, b, a), other, axis=1)
                    out[i], out[i + stride] = jnp.where(low, a, moved), jnp.where(low, moved, b)
    return jnp.concatenate(out, axis=0)


def kernel(sizes, sr_hbm, si_hbm, gr_hbm, gi_hbm, o_ref, *scratch):
    nfar, nnear, high, order, lows = sizes
    (
        st_ref, lr_ref, li_ref, gr_ref, gi_ref, kf_ref, km_ref, w_ref,
        send0, send1, send2, recv0, recv1, recv2,
        x_ref, send_sem, recv_sem, load_sem, ready_sem,
    ) = scratch
    far, near = lax.axis_index("far"), lax.axis_index("near")
    core, side = near % 2, far % 2
    upper = order // high
    rest = order // upper
    rows = high * order
    fine = lows // nnear
    eight = fine // 2

    def flips(at, bits):
        found = []
        for mask in range(2**bits):
            found.append(sum((at // 2**i % 2 + mask // 2**i % 2) % 2 * 2**i for i in range(bits)))
        return found

    fars, nears = flips(far, 2), flips(near, 3)
    others = [(a, b) for a in range(nfar) for b in range(nnear) if a + b]
    others.sort(key=lambda ab: -(ab[0] + ab[1] // 4 + ab[1] // 2 % 2))

    barrier = pltpu.get_barrier_semaphore()
    close = [(a, b) for a, b in others if a * b == 0]
    distant = [(a, b) for a, b in others if a * b]
    for a, b in close:
        pl.semaphore_signal(
            barrier, inc=1, device_id=(fars[a], nears[b]), device_id_type=pl.DeviceIdType.MESH
        )
    first = [
        pltpu.make_async_copy(gr_hbm.at[0, pl.ds(0, 2), 0], lr_ref, load_sem.at[0]),
        pltpu.make_async_copy(gi_hbm.at[0, pl.ds(0, 2), 0], li_ref, load_sem.at[1]),
        pltpu.make_async_copy(sr_hbm, st_ref.at[0], load_sem.at[2]),
        pltpu.make_async_copy(si_hbm, st_ref.at[1], load_sem.at[3]),
    ]
    gates = [
        pltpu.make_async_copy(gr_hbm, gr_ref, load_sem.at[4]),
        pltpu.make_async_copy(gi_hbm, gi_ref, load_sem.at[5]),
    ]
    for load in first + gates:
        load.start()

    def remote(stage, source, target, to, group=0):
        return pltpu.make_async_remote_copy(
            src_ref=source,
            dst_ref=target,
            send_sem=send_sem.at[stage],
            recv_sem=recv_sem.at[stage + group],
            device_id=to,
            device_id_type=pl.DeviceIdType.MESH,
        )

    def settle(ref, sem):
        pltpu.make_async_copy(ref, ref, sem).wait()

    def gate(s, which):
        return gr_ref[s // 4, s % 4, which], gi_ref[s // 4, s % 4, which]

    def tops_after_mids(s):
        left = parts(complex_matrix(*gate(s, 2)))
        zero = jnp.zeros((upper, order), jnp.float32)
        for t in range(rest):
            blocks = []
            for ref in (gr_ref, gi_ref):
                mid = ref[s // 4, s % 4, 1, pl.ds(t, upper, stride=rest), :]
                for h in range(high):
                    blocks.append(jnp.concatenate([mid if g == h else zero for g in range(high)], axis=1))
            out = dot(left, parts(jnp.concatenate(blocks, axis=0)))
            for c in range(2):
                for h in range(high):
                    for g in range(high):
                        kf_ref[c, g, h, pl.ds(t, upper, stride=rest), :] = out[
                            c * order + h * upper : c * order + (h + 1) * upper, g * order : (g + 1) * order
                        ]
        return tuple(
            jnp.concatenate([kf_ref[c, g].reshape(rows, order) for g in range(high)], axis=1) for c in range(2)
        )

    def put_high(at, pair):
        km_ref[at, 0], km_ref[at, 1] = parts(jnp.concatenate(pair, axis=0))

    def high_of(at):
        return km_ref[at, 0], km_ref[at, 1]

    def rows_of(at, half):
        places = [pl.ds(pl.multiple_of(half * order, order) + c * rows, order) for c in range(2)]
        return tuple(jnp.concatenate([km_ref[at, p, place] for place in places], axis=0) for p in range(2))

    def rows_with(at, half):
        places = [
            pl.ds(pl.multiple_of(half * upper, upper) + (c * high + k) * order, upper)
            for c in range(2)
            for k in range(high)
        ]
        return tuple(jnp.concatenate([km_ref[at, p, place] for place in places], axis=0) for p in range(2))

    def put_low(at, pair, finely):
        wide = complex_matrix(*pair).T
        if finely:
            wide = jnp.concatenate(
                [
                    wide[((c * nnear + b) * 2 + k) * eight : ((c * nnear + b) * 2 + k + 1) * eight]
                    for c in range(2)
                    for k in range(2)
                    for b in range(nnear)
                ],
                axis=0,
            )
        w_ref[at, 0], w_ref[at, 1] = parts(wide)

    def low_gate(at, pair):
        out = dot(parts(jnp.concatenate(pair, axis=1)), (w_ref[at, 0], w_ref[at, 1]))
        return out[:, :lows], out[:, lows:]

    def traded(pair, swaps):
        return tuple(trade(x, swaps) for x in pair)

    first[0].wait()
    first[1].wait()
    last = tuple(
        jnp.concatenate([ref[1, pl.ds(k, nnear, stride=fine), :] for k in range(fine)], axis=0)
        for ref in (lr_ref, li_ref)
    )
    low = parts(complex_matrix(*product(last, (lr_ref[0], li_ref[0]))))
    first[2].wait()
    first[3].wait()
    state = dot(parts(jnp.concatenate([st_ref[0], st_ref[1]], axis=1)), low, ((1,), (1,)))
    pair = traded((state[:, :lows], state[:, lows:]), ((64, 64), (32, 32), (16, 16), (8, 8)))
    for c in range(2):
        for h in range(high):
            for k in range(fine):
                at = (h * fine + k) * eight
                send0[k * high + h, c] = pair[c][at : at + eight]
    pl.semaphore_wait(barrier, len(close))
    for a in range(1, nfar):
        pl.semaphore_signal(ready_sem, inc=1, device_id=(fars[a], near), device_id_type=pl.DeviceIdType.MESH)
    me = far * nnear + near
    for peers in (close, distant):
        if peers is distant:
            pl.semaphore_wait(ready_sem, nfar - 1)
        for a, b in peers:
            remote(0, send0.at[fars[a] * nnear + nears[b]], recv0.at[me], (fars[a], nears[b]), 3 * a).start()
    recv0[me] = send0[me]

    for load in gates:
        load.wait()
    put_high(0, tops_after_mids(0))
    put_high(1, tops_after_mids(2))
    put_high(1, complex_rows(high_of(1), split(tops_after_mids(1))))
    put_high(2, tops_after_mids(3))
    put_high(3, tops_after_mids(4))
    put_high(4, tops_after_mids(6))
    put_high(4, complex_rows(high_of(4), split(tops_after_mids(5))))

    def keep(at, pair):
        count = pair[0].shape[0]
        place = pl.ds(pl.multiple_of(at * count, count), count)
        x_ref[0, place], x_ref[1, place] = parts(jnp.concatenate(pair, axis=1))

    for a in range(nfar):
        landed = recv0.at[pl.ds(fars[a] * nnear, nnear - 1 if a == 0 else nnear)]
        settle(landed, recv_sem.at[3 * a])
        pair = tuple(recv0[pl.ds(fars[a] * nnear, nnear), c].reshape(rows // nfar, lows) for c in range(2))
        keep(fars[a], traded(pair, ((32, 32), (16, 16), (8, 8))))
    pair = complex_rows(high_of(0), (x_ref[0], x_ref[1]))
    pair = complex_rows(high_of(1), split(traded(pair, ((64, 32), (32, 16), (16, 8)))))
    ready = split(traded(pair, ((128, 4), (64, 2), (32, 1))))
    send1[0], send1[1] = complex_rows(rows_with(2, 1 - core), ready)
    remote(1, send1, recv1, (far, nears[1])).start()
    keep(core, traded(complex_rows(rows_with(2, core), ready), ((64, 64),)))
    settle(recv1, recv_sem.at[1])
    keep(1 - core, traded((recv1[0], recv1[1]), ((64, 64),)))
    pair = complex_rows(high_of(3), (x_ref[0], x_ref[1]))
    ready = split(traded(pair, ((64, 4), (32, 2), (16, 1))))
    thin = rows // nnear // 2
    here = far * (nnear // 2) + near // 2
    same = side == core
    for h in (1, 0):
        top = (near // 4 + h) % 2
        pair = traded(complex_rows(rows_of(4, top), ready), ((16, 64),))
        for c in range(2):
            for b in range(nnear // 2):
                for k in range(2):
                    at = (b * 2 + k) * thin
                    send2[k * nnear + top * (nnear // 2) + b, c] = pair[c][at : at + thin]
        for b in (2, 3, 1, 0):
            for a in (1, 0):
                to = ((far // 2 + a) % 2 * 2 + core, nears[4 * h + b])
                copy = remote(2, send2.at[to[0] // 2 * nnear + to[1]], recv2.at[here], to)
                if a + b + h:
                    copy.start()
                else:
                    @pl.when(jnp.logical_not(same))
                    def _():
                        copy.start()

                    @pl.when(same)
                    def _():
                        recv2[here] = send2[far // 2 * nnear + near]

    put_high(5, tops_after_mids(7))
    put_low(0, product(gate(5, 0), product(gate(4, 0), product(gate(3, 0), gate(2, 0)))), True)
    put_low(1, product(gate(7, 0), gate(6, 0)), False)

    count = 2 * nnear

    @pl.when(same)
    def _():
        settle(recv2.at[pl.ds(0, count - 1)], recv_sem.at[2])

    @pl.when(jnp.logical_not(same))
    def _():
        settle(recv2, recv_sem.at[2])

    pair = tuple(recv2[:, c].reshape(rows, lows) for c in range(2))
    pair = low_gate(0, traded(pair, ((128, 64), (64, 4), (32, 2), (16, 1))))
    pair = low_gate(1, traded(pair, ((64, 64), (32, 32), (16, 16))))
    pair = tuple(
        jnp.concatenate(
            [x[(k * nnear + b) * thin : (k * nnear + b + 1) * thin] for b in range(nnear) for k in range(2)], axis=0
        )
        for x in pair
    )
    o_ref[0], o_ref[1] = complex_rows(high_of(5), split(pair))

    settle(send0.at[pl.ds(0, nfar * nnear - 1)], send_sem.at[0])
    settle(send1, send_sem.at[1])

    @pl.when(same)
    def _():
        settle(send2.at[pl.ds(0, count - 1)], send_sem.at[2])

    @pl.when(jnp.logical_not(same))
    def _():
        settle(send2, send_sem.at[2])


def one_kernel(nfar, nnear, state_real, state_imag, gate_real, gate_imag):
    shape = state_real.shape
    high, order, lows = shape[2:]
    rows = high * order
    blocks = (
        (nfar * nnear, 2, rows // nfar // nnear, lows),
        (2, rows // 2, lows),
        (2 * nnear, 2, rows // nnear // 2, lows),
    )
    buffers = [pltpu.VMEM(block, jnp.float32) for block in blocks]
    vmem = pl.BlockSpec(memory_space=pltpu.VMEM)
    anywhere = pl.BlockSpec(memory_space=pl.ANY)
    result = pltpu.VMEM((rows, lows), jnp.float32)
    both = pl.pallas_call(
        functools.partial(kernel, (nfar, nnear, high, order, lows)),
        out_shape=pltpu.VMEM((2, rows, lows), jnp.float32),
        in_specs=[anywhere] * 4,
        out_specs=vmem,
        scratch_shapes=[
            pltpu.VMEM((2, rows, lows), jnp.float32),
            pltpu.VMEM((2, order, order), jnp.float32),
            pltpu.VMEM((2, order, order), jnp.float32),
            pltpu.VMEM(gate_real.shape, jnp.float32),
            pltpu.VMEM(gate_imag.shape, jnp.float32),
            pltpu.VMEM((2, high, high, order, order), jnp.float32),
            pltpu.VMEM((6, 2, 2 * rows, rows), jnp.bfloat16),
            pltpu.VMEM((2, 2, 2 * lows, 2 * lows), jnp.bfloat16),
        ]
        + buffers
        + buffers
        + [
            pltpu.VMEM((2, rows, 2 * lows), jnp.bfloat16),
            pltpu.SemaphoreType.DMA((3,)),
            pltpu.SemaphoreType.DMA((3 * nfar,)),
            pltpu.SemaphoreType.DMA((6,)),
            pltpu.SemaphoreType.REGULAR,
        ],
        compiler_params=pltpu.CompilerParams(collective_id=0, has_side_effects=True),
    )(
        state_real.reshape(rows, lows),
        state_imag.reshape(rows, lows),
        gate_real,
        gate_imag,
    )
    return both[0].reshape(shape), both[1].reshape(shape)


def solution(mesh):
    nfar, nnear = mesh.shape["far"], mesh.shape["near"]

    def body(state_real, state_imag, gate_real, gate_imag):
        high, order, lows = state_real.shape[2:]
        fits = high == 2 and nfar == high**2 and nnear == high**3 and order == lows and gate_real.shape[0] == 2
        fits = fits and lows == 2 * nnear * 8
        if not fits:
            return on_device(state_real, state_imag, gate_real, gate_imag)
        return one_kernel(nfar, nnear, state_real, state_imag, gate_real, gate_imag)

    return jax.shard_map(
        body,
        mesh=mesh,
        in_specs=(P("far", "near", None, None, None), P("far", "near", None, None, None), P(), P()),
        out_specs=(P("far", "near", None, None, None), P("far", "near", None, None, None)),
        check_vma=False,
    )
```

```python
import functools

import jax
import jax.numpy as jnp
from jax import lax
from jax.experimental import pallas as pl
from jax.experimental.pallas import tpu as pltpu
from jax.sharding import PartitionSpec as P


def gate_low(x, g):
    return jnp.einsum(
        "...l,jl->...j", x, g, precision=lax.Precision.HIGHEST, preferred_element_type=jnp.float32
    )


def gate_mid(x, g):
    return jnp.einsum(
        "...ml,jm->...jl", x, g, precision=lax.Precision.HIGHEST, preferred_element_type=jnp.float32
    )


def gate_top(x, g):
    high, width, lows = (x.shape[-3], x.shape[-2], x.shape[-1])
    upper = g.shape[0] // high
    lead = x.shape[:-3]
    viewed = x.reshape(lead + (high, upper, width // upper, lows))
    matrix = g.reshape((g.shape[0], high, upper))
    out = jnp.einsum(
        "...hkrl,jhk->...jrl",
        viewed,
        matrix,
        precision=lax.Precision.HIGHEST,
        preferred_element_type=jnp.float32,
    )
    return out.reshape(lead + (high, width, lows))


def complex_gate(form, real, imag, greal, gimag):
    new_real = form(real, greal) - form(imag, gimag)
    new_imag = form(imag, greal) + form(real, gimag)
    return (new_real, new_imag)


def merged_rows(x):
    return x.reshape((1, 1, x.shape[2] * x.shape[3], x.shape[4]))


def on_device(state_real, state_imag, gate_real, gate_imag):
    real, imag = (state_real, state_imag)
    forms = (gate_low, gate_mid, gate_top)
    shape = state_real.shape
    for rnd in range(gate_real.shape[0]):
        for section in range(4):
            if section == 2:
                order = [1, 0, 2]
            else:
                order = [0, 1, 2]
            early = []
            later = order[len(early) :]
            pair = (real, imag)
            if section == 0:
                moved = (
                    lax.all_to_all(
                        merged_rows(pair[0]), "far", split_axis=2, concat_axis=2, tiled=True
                    ),
                    lax.all_to_all(
                        merged_rows(pair[1]), "far", split_axis=2, concat_axis=2, tiled=True
                    ),
                )
                pair = (moved[0].reshape(shape), moved[1].reshape(shape))
            elif section == 1:
                pair = (
                    lax.all_to_all(pair[0], "near", split_axis=3, concat_axis=3, tiled=True),
                    lax.all_to_all(pair[1], "near", split_axis=3, concat_axis=3, tiled=True),
                )
            elif section == 2:
                pair = (
                    lax.all_to_all(pair[0], "near", split_axis=4, concat_axis=4, tiled=True),
                    lax.all_to_all(pair[1], "near", split_axis=4, concat_axis=4, tiled=True),
                )
            else:
                moved = (
                    lax.all_to_all(
                        merged_rows(pair[0]), "near", split_axis=2, concat_axis=2, tiled=True
                    ),
                    lax.all_to_all(
                        merged_rows(pair[1]), "near", split_axis=2, concat_axis=2, tiled=True
                    ),
                )
                pair = (moved[0].reshape(shape), moved[1].reshape(shape))
            for which in later:
                pair = complex_gate(
                    forms[which],
                    pair[0],
                    pair[1],
                    gate_real[rnd, section, which],
                    gate_imag[rnd, section, which],
                )
            real, imag = pair
    return (real, imag)


def parts(x):
    first = x.astype(jnp.bfloat16)
    return first, (x - first.astype(jnp.float32)).astype(jnp.bfloat16)


def dot(a, b, dims=((1,), (0,))):
    def product(x, y):
        return lax.dot_general(x, y, (dims, ((), ())), preferred_element_type=jnp.float32)

    return product(a[0], b[0]) + (product(a[0], b[1]) + product(a[1], b[0]))


def split(pair):
    return parts(jnp.concatenate(pair, axis=1))


def complex_rows(stacked, pair):
    out = dot(stacked, pair)
    n, w = out.shape[0] // 2, out.shape[1] // 2
    return out[:n, :w] - out[n:, w:], out[n:, :w] + out[:n, w:]


def product(a, b):
    return complex_rows(parts(jnp.concatenate(a, axis=0)), split(b))


def complex_matrix(re, im):
    return jnp.concatenate(
        [jnp.concatenate([re, -im], axis=1), jnp.concatenate([im, re], axis=1)], axis=0
    )


def trade(x, swaps):
    unit = 8
    rows, lanes = x.shape
    at = lax.broadcasted_iota(jnp.int32, (unit, lanes), 1)
    steps = []
    for row, lane in swaps:
        low = lax.rem(lax.div(at, lane), 2) == 0
        steps.append((row // unit, low, jnp.where(low, at + lane, at - lane)))
    out = [None] * (rows // unit)
    for base in range(rows // unit):
        if any(base // stride % 2 for stride, _, _ in steps):
            continue
        group = [base]
        for stride, _, _ in steps:
            group = group + [i + stride for i in group]
        for i in group:
            out[i] = x[i * unit : (i + 1) * unit]
        for stride, low, other in steps:
            for i in group:
                if i // stride % 2 == 0:
                    a, b = out[i], out[i + stride]
                    moved = jnp.take_along_axis(jnp.where(low, b, a), other, axis=1)
                    out[i], out[i + stride] = jnp.where(low, a, moved), jnp.where(low, moved, b)
    return jnp.concatenate(out, axis=0)


def kernel(sizes, sr_hbm, si_hbm, gr_hbm, gi_hbm, o_ref, *scratch):
    nfar, nnear, high, order, lows = sizes
    (
        st_ref, lr_ref, li_ref, gr_ref, gi_ref, kf_ref, km_ref, w_ref,
        send0, send1, send2, recv0, recv1, recv2,
        x_ref, relay_ref, send_sem, recv_sem, load_sem, ready_sem,
    ) = scratch
    far, near = lax.axis_index("far"), lax.axis_index("near")
    core, side = near % 2, far % 2
    upper = order // high
    rest = order // upper
    rows = high * order
    fine = lows // nnear
    eight = fine // 2

    def flips(at, bits):
        found = []
        for mask in range(2**bits):
            found.append(sum((at // 2**i % 2 + mask // 2**i % 2) % 2 * 2**i for i in range(bits)))
        return found

    fars, nears = flips(far, 2), flips(near, 3)
    others = [(a, b) for a in range(nfar) for b in range(nnear) if a + b]
    others.sort(key=lambda ab: -(ab[0] + ab[1] // 4 + ab[1] // 2 % 2))

    relayed = (1, 2)
    barrier = pltpu.get_barrier_semaphore()
    close = [(a, b) for a, b in others if a * b == 0]
    distant = [(a, b) for a, b in others if a * b]
    for a, b in close:
        pl.semaphore_signal(
            barrier, inc=1, device_id=(fars[a], nears[b]), device_id_type=pl.DeviceIdType.MESH
        )
    first = [
        pltpu.make_async_copy(gr_hbm.at[0, pl.ds(0, 2), 0], lr_ref, load_sem.at[0]),
        pltpu.make_async_copy(gi_hbm.at[0, pl.ds(0, 2), 0], li_ref, load_sem.at[1]),
        pltpu.make_async_copy(sr_hbm, st_ref.at[0], load_sem.at[2]),
        pltpu.make_async_copy(si_hbm, st_ref.at[1], load_sem.at[3]),
    ]
    gates = [
        pltpu.make_async_copy(gr_hbm, gr_ref, load_sem.at[4]),
        pltpu.make_async_copy(gi_hbm, gi_ref, load_sem.at[5]),
    ]
    for load in first + gates:
        load.start()

    def remote(stage, source, target, to, at):
        return pltpu.make_async_remote_copy(
            src_ref=source,
            dst_ref=target,
            send_sem=send_sem.at[stage],
            recv_sem=recv_sem.at[at],
            device_id=to,
            device_id_type=pl.DeviceIdType.MESH,
        )

    def settle(ref, sem):
        pltpu.make_async_copy(ref, ref, sem).wait()

    def gate(s, which):
        return gr_ref[s // 4, s % 4, which], gi_ref[s // 4, s % 4, which]

    def tops_after_mids(s):
        left = parts(complex_matrix(*gate(s, 2)))
        zero = jnp.zeros((upper, order), jnp.float32)
        for t in range(rest):
            blocks = []
            for ref in (gr_ref, gi_ref):
                mid = ref[s // 4, s % 4, 1, pl.ds(t, upper, stride=rest), :]
                for h in range(high):
                    blocks.append(jnp.concatenate([mid if g == h else zero for g in range(high)], axis=1))
            out = dot(left, parts(jnp.concatenate(blocks, axis=0)))
            for c in range(2):
                for h in range(high):
                    for g in range(high):
                        kf_ref[c, g, h, pl.ds(t, upper, stride=rest), :] = out[
                            c * order + h * upper : c * order + (h + 1) * upper, g * order : (g + 1) * order
                        ]
        return tuple(
            jnp.concatenate([kf_ref[c, g].reshape(rows, order) for g in range(high)], axis=1) for c in range(2)
        )

    def put_high(at, pair):
        km_ref[at, 0], km_ref[at, 1] = parts(jnp.concatenate(pair, axis=0))

    def high_of(at):
        return km_ref[at, 0], km_ref[at, 1]

    def rows_of(at, half):
        places = [pl.ds(pl.multiple_of(half * order, order) + c * rows, order) for c in range(2)]
        return tuple(jnp.concatenate([km_ref[at, p, place] for place in places], axis=0) for p in range(2))

    def rows_with(at, half):
        places = [
            pl.ds(pl.multiple_of(half * upper, upper) + (c * high + k) * order, upper)
            for c in range(2)
            for k in range(high)
        ]
        return tuple(jnp.concatenate([km_ref[at, p, place] for place in places], axis=0) for p in range(2))

    def put_low(at, pair, finely):
        wide = complex_matrix(*pair).T
        if finely:
            wide = jnp.concatenate(
                [
                    wide[((c * nnear + b) * 2 + k) * eight : ((c * nnear + b) * 2 + k + 1) * eight]
                    for c in range(2)
                    for k in range(2)
                    for b in range(nnear)
                ],
                axis=0,
            )
        w_ref[at, 0], w_ref[at, 1] = parts(wide)

    def low_gate(at, pair):
        out = dot(parts(jnp.concatenate(pair, axis=1)), (w_ref[at, 0], w_ref[at, 1]))
        return out[:, :lows], out[:, lows:]

    def traded(pair, swaps):
        return tuple(trade(x, swaps) for x in pair)

    first[0].wait()
    first[1].wait()
    last = tuple(
        jnp.concatenate([ref[1, pl.ds(k, nnear, stride=fine), :] for k in range(fine)], axis=0)
        for ref in (lr_ref, li_ref)
    )
    low = parts(complex_matrix(*product(last, (lr_ref[0], li_ref[0]))))
    first[2].wait()
    first[3].wait()
    state = dot(parts(jnp.concatenate([st_ref[0], st_ref[1]], axis=1)), low, ((1,), (1,)))
    pair = traded((state[:, :lows], state[:, lows:]), ((64, 64), (32, 32), (16, 16), (8, 8)))
    for c in range(2):
        for h in range(high):
            for k in range(fine):
                at = (h * fine + k) * eight
                send0[k * high + h, c] = pair[c][at : at + eight]
    pl.semaphore_wait(barrier, len(close))
    for a in range(1, nfar):
        pl.semaphore_signal(ready_sem, inc=1, device_id=(fars[a], near), device_id_type=pl.DeviceIdType.MESH)
    me = far * nnear + near
    for a, b in close:
        if a:
            for i, k in enumerate(relayed):
                block = send0.at[fars[a] * nnear + nears[k]]
                remote(3, block, relay_ref.at[far, i], (fars[a], near), 1).start()
        remote(0, send0.at[fars[a] * nnear + nears[b]], recv0.at[me], (fars[a], nears[b]), 3 * a).start()
    pl.semaphore_wait(ready_sem, nfar - 1)
    for a, b in distant:
        if b not in relayed:
            remote(0, send0.at[fars[a] * nnear + nears[b]], recv0.at[me], (fars[a], nears[b]), 3 * a).start()
    recv0[me] = send0[me]

    for load in gates:
        load.wait()
    put_high(0, tops_after_mids(0))
    put_high(1, tops_after_mids(2))
    put_high(1, complex_rows(high_of(1), split(tops_after_mids(1))))
    put_high(2, tops_after_mids(3))
    settle(relay_ref.at[pl.ds(0, nfar - 1)], recv_sem.at[1])
    for a in range(1, nfar):
        for i, k in enumerate(relayed):
            remote(3, relay_ref.at[fars[a], i], recv0.at[fars[a] * nnear + near], (far, nears[k]), 3 * a).start()
    put_high(3, tops_after_mids(4))
    put_high(4, tops_after_mids(6))
    put_high(4, complex_rows(high_of(4), split(tops_after_mids(5))))

    def keep(at, pair):
        count = pair[0].shape[0]
        place = pl.ds(pl.multiple_of(at * count, count), count)
        x_ref[0, place], x_ref[1, place] = parts(jnp.concatenate(pair, axis=1))

    for a in range(nfar):
        landed = recv0.at[pl.ds(fars[a] * nnear, nnear - 1 if a == 0 else nnear)]
        settle(landed, recv_sem.at[3 * a])
        pair = tuple(recv0[pl.ds(fars[a] * nnear, nnear), c].reshape(rows // nfar, lows) for c in range(2))
        keep(fars[a], traded(pair, ((32, 32), (16, 16), (8, 8))))
    pair = complex_rows(high_of(0), (x_ref[0], x_ref[1]))
    pair = complex_rows(high_of(1), split(traded(pair, ((64, 32), (32, 16), (16, 8)))))
    ready = split(traded(pair, ((128, 4), (64, 2), (32, 1))))
    send1[0], send1[1] = complex_rows(rows_with(2, 1 - core), ready)
    remote(1, send1, recv1, (far, nears[1]), 2).start()
    keep(core, traded(complex_rows(rows_with(2, core), ready), ((64, 64),)))
    settle(recv1, recv_sem.at[2])
    keep(1 - core, traded((recv1[0], recv1[1]), ((64, 64),)))
    pair = complex_rows(high_of(3), (x_ref[0], x_ref[1]))
    ready = split(traded(pair, ((64, 4), (32, 2), (16, 1))))
    thin = rows // nnear // 2
    here = far * (nnear // 2) + near // 2
    same = side == core
    for h in (1, 0):
        top = (near // 4 + h) % 2
        pair = traded(complex_rows(rows_of(4, top), ready), ((16, 64),))
        for c in range(2):
            for b in range(nnear // 2):
                for k in range(2):
                    at = (b * 2 + k) * thin
                    send2[k * nnear + top * (nnear // 2) + b, c] = pair[c][at : at + thin]
        for b in (2, 3, 1, 0):
            for a in (1, 0):
                to = ((far // 2 + a) % 2 * 2 + core, nears[4 * h + b])
                copy = remote(2, send2.at[to[0] // 2 * nnear + to[1]], recv2.at[here], to, 4)
                if a + b + h:
                    copy.start()
                else:
                    @pl.when(jnp.logical_not(same))
                    def _():
                        copy.start()

                    @pl.when(same)
                    def _():
                        recv2[here] = send2[far // 2 * nnear + near]

    put_high(5, tops_after_mids(7))
    put_low(0, product(gate(5, 0), product(gate(4, 0), product(gate(3, 0), gate(2, 0)))), True)
    put_low(1, product(gate(7, 0), gate(6, 0)), False)

    count = 2 * nnear

    @pl.when(same)
    def _():
        settle(recv2.at[pl.ds(0, count - 1)], recv_sem.at[4])

    @pl.when(jnp.logical_not(same))
    def _():
        settle(recv2, recv_sem.at[4])

    pair = tuple(recv2[:, c].reshape(rows, lows) for c in range(2))
    pair = low_gate(0, traded(pair, ((128, 64), (64, 4), (32, 2), (16, 1))))
    pair = low_gate(1, traded(pair, ((64, 64), (32, 32), (16, 16))))
    pair = tuple(
        jnp.concatenate(
            [x[(k * nnear + b) * thin : (k * nnear + b + 1) * thin] for b in range(nnear) for k in range(2)], axis=0
        )
        for x in pair
    )
    o_ref[0], o_ref[1] = complex_rows(high_of(5), split(pair))

    passed = (nfar - 1) * len(relayed)
    settle(send0.at[pl.ds(0, nfar * nnear - 1 - passed)], send_sem.at[0])
    settle(send0.at[pl.ds(0, 2 * passed)], send_sem.at[3])
    settle(send1, send_sem.at[1])

    @pl.when(same)
    def _():
        settle(send2.at[pl.ds(0, count - 1)], send_sem.at[2])

    @pl.when(jnp.logical_not(same))
    def _():
        settle(send2, send_sem.at[2])


def one_kernel(nfar, nnear, state_real, state_imag, gate_real, gate_imag):
    shape = state_real.shape
    high, order, lows = shape[2:]
    rows = high * order
    blocks = (
        (nfar * nnear, 2, rows // nfar // nnear, lows),
        (2, rows // 2, lows),
        (2 * nnear, 2, rows // nnear // 2, lows),
    )
    buffers = [pltpu.VMEM(block, jnp.float32) for block in blocks]
    vmem = pl.BlockSpec(memory_space=pltpu.VMEM)
    anywhere = pl.BlockSpec(memory_space=pl.ANY)
    result = pltpu.VMEM((rows, lows), jnp.float32)
    both = pl.pallas_call(
        functools.partial(kernel, (nfar, nnear, high, order, lows)),
        out_shape=pltpu.VMEM((2, rows, lows), jnp.float32),
        in_specs=[anywhere] * 4,
        out_specs=vmem,
        scratch_shapes=[
            pltpu.VMEM((2, rows, lows), jnp.float32),
            pltpu.VMEM((2, order, order), jnp.float32),
            pltpu.VMEM((2, order, order), jnp.float32),
            pltpu.VMEM(gate_real.shape, jnp.float32),
            pltpu.VMEM(gate_imag.shape, jnp.float32),
            pltpu.VMEM((2, high, high, order, order), jnp.float32),
            pltpu.VMEM((6, 2, 2 * rows, rows), jnp.bfloat16),
            pltpu.VMEM((2, 2, 2 * lows, 2 * lows), jnp.bfloat16),
        ]
        + buffers
        + buffers
        + [
            pltpu.VMEM((2, rows, 2 * lows), jnp.bfloat16),
            pltpu.VMEM((nfar, 2) + blocks[0][1:], jnp.float32),
            pltpu.SemaphoreType.DMA((4,)),
            pltpu.SemaphoreType.DMA((3 * nfar - 2,)),
            pltpu.SemaphoreType.DMA((6,)),
            pltpu.SemaphoreType.REGULAR,
        ],
        compiler_params=pltpu.CompilerParams(collective_id=0, has_side_effects=True),
    )(
        state_real.reshape(rows, lows),
        state_imag.reshape(rows, lows),
        gate_real,
        gate_imag,
    )
    return both[0].reshape(shape), both[1].reshape(shape)


def solution(mesh):
    nfar, nnear = mesh.shape["far"], mesh.shape["near"]

    def body(state_real, state_imag, gate_real, gate_imag):
        high, order, lows = state_real.shape[2:]
        fits = high == 2 and nfar == high**2 and nnear == high**3 and order == lows and gate_real.shape[0] == 2
        fits = fits and lows == 2 * nnear * 8
        if not fits:
            return on_device(state_real, state_imag, gate_real, gate_imag)
        return one_kernel(nfar, nnear, state_real, state_imag, gate_real, gate_imag)

    return jax.shard_map(
        body,
        mesh=mesh,
        in_specs=(P("far", "near", None, None, None), P("far", "near", None, None, None), P(), P()),
        out_specs=(P("far", "near", None, None, None), P("far", "near", None, None, None)),
        check_vma=False,
    )
```
